256 devices in a mesh: lat: 8 (over x_lo, y), lon: 32 (over z, x_hi, core).
Axes of the slice: x: 4 (x_hi: 2, x_lo: 2; x = x_hi * 2 + x_lo), y: 4, z: 8, core: 2. Of those that a mesh axis runs over, the one named last changes fastest.
Arguments:
- activations: bfloat16 [4, 32, 2880, 512], P(None, 'lat', 'lon'), may hold values from -48 to 48
- upstream: bfloat16 [4, 32, 2880, 512], P(None, 'lat', 'lon'), may hold values from -6 to 6
- master: float32 [512, 9, 512], P(('lat', 'lon')), may hold values from -0.09375 to 0.09375
- moment_one: float32 [512, 9, 512], P(('lat', 'lon')), may hold values from -2.5 to 2.5
- moment_two: float32 [512, 9, 512], P(('lat', 'lon')), may hold values from 0.01 to 1
Outputs:
- input_grad: bfloat16 [4, 32, 2880, 512], P(None, 'lat', 'lon')
- new_weights: bfloat16 [512, 9, 512], replicated
- new_master: float32 [512, 9, 512], P(('lat', 'lon'))
- new_moment_one: float32 [512, 9, 512], P(('lat', 'lon'))
- new_moment_two: float32 [512, 9, 512], P(('lat', 'lon'))
- clipped_grad: float32 [512, 9, 512], P(('lat', 'lon'))
The draws below stay inside these ranges and needn't reach their ends.
All inputs are finite; a program needn't handle non-finite values.
Results may differ from the reference program's by a relative error of at most 0.0049.
Values may be sent and summed in bfloat16 or wider, within the bound.
A program may use at most 128 MiB of HBM per device.

```python
import math
import jax
import jax.numpy as jnp
from jax import lax

CIN = 512
COUT = 512
TAPS = 9
BATCH = 4
COLS_DEV = 90
NLAT = 32
NLON = 2880
N_LON = 32


def draw_activations(key, part):
    key_noise, key_spread = jax.random.split(key, 2)
    key_pair = jax.random.fold_in(key, 77)
    channel_ramp = jnp.sqrt(1.0 + 2.0 * jnp.arange(CIN, dtype=jnp.float32) / CIN)
    spread = jnp.exp(jax.random.uniform(key_spread, (CIN,), jnp.float32, 0.0, jnp.log(10.0)))
    chan_scale = channel_ramp * spread / 4.0
    pairing = jax.random.permutation(key_pair, N_LON)
    col_block = jnp.arange(NLON, dtype=jnp.int32) // COLS_DEV
    chan_block = jnp.arange(CIN, dtype=jnp.int32) // (CIN // N_LON)
    heavy = pairing[col_block][:, None] == chan_block[None, :]
    boost = jnp.where(heavy, 6.0, 1.0).astype(jnp.float32)[None, None, :, :]
    noise_draw = jax.random.normal(key_noise, (BATCH, NLAT, NLON, CIN), jnp.float32)
    values = noise_draw * chan_scale * boost
    return jnp.clip(values, -48.0, 48.0).astype(jnp.bfloat16)


def level_of(key, dims, cuts, low, top_value):
    factor_of = 1.0
    for dim, parts in cuts:
        draws = jax.random.uniform(jax.random.fold_in(jax.random.fold_in(key, 6), dim), (parts,), jnp.float32, low / len(cuts), top_value / len(cuts))
        factor_of = factor_of * jnp.repeat(jnp.exp(draws), dims[dim] // parts).reshape((-1,) + (1,) * (len(dims) - 1 - dim))
    return factor_of


def scatter_about(stream_key, extent, deviation, limit, cuts=(), kind=jnp.bfloat16):
    level = level_of(stream_key, extent, cuts, -0.22, 0.18) if cuts else 1.0
    result = jax.random.normal(stream_key, extent, jnp.float32) * deviation * level
    return jnp.minimum(jnp.maximum(result, -limit), limit).astype(kind)


def setup_inputs(seed: int = 0) -> dict:
    key_list = jax.random.split(jax.random.key(seed), 6)
    activations = draw_activations(jax.random.fold_in(key_list[5], 71), 0)
    upstream = scatter_about(key_list[1], (BATCH, NLAT, NLON, COUT), 1.0, 6.0, ((1, 8), (2, 32)))
    master = scatter_about(key_list[2], (CIN, TAPS, COUT), (CIN * TAPS) ** -0.5, 0.09375, ((0, 256),), jnp.float32)
    moment_one = scatter_about(key_list[3], (CIN, TAPS, COUT), 0.3, 2.5, ((0, 256),), jnp.float32)
    moment_two = jnp.clip(jnp.exp(math.log(1.0) - 4.6051702 * jax.random.uniform(key_list[4], (CIN, TAPS, COUT), jnp.float32) ** level_of(key_list[4], (CIN, TAPS, COUT), ((0, 256),), -0.2, 0.2)), 0.01, 1.0)
    return {"activations": activations, "upstream": upstream, "master": master, "moment_one": moment_one, "moment_two": moment_two}


learn_rate = 0.01
beta_one = 0.9
beta_two = 0.999
adam_eps = 1e-08
decay_rate = 0.1
step_count = 10.0
norm_eps = 1e-06

def widen_field(field):
    padded = jnp.pad(field, ((1, 1), (0, 0), (0, 0)))
    return jnp.concatenate([padded[:, -1:, :], padded, padded[:, :1, :]], axis=1)

def reference(activations, upstream, master, moment_one, moment_two):
    weights = master.astype(jnp.bfloat16)

    def one_sample(grad_total, sample):
        act_one, up_one = sample
        act_wide = widen_field(act_one)
        up_wide = widen_field(up_one)
        up_flat = up_one.reshape(-1, COUT)
        data_sum = jnp.zeros((NLAT * NLON, CIN), jnp.float32)
        tap_parts = []
        for tap_index in range(9):
            row_off, col_off = divmod(tap_index, 3)
            shifted = up_wide[2 - row_off:2 - row_off + NLAT, 2 - col_off:2 - col_off + NLON, :].reshape(-1, COUT)
            data_sum = data_sum + jnp.dot(shifted, weights[:, tap_index, :].T, preferred_element_type=jnp.float32)
            act_tap = act_wide[row_off:row_off + NLAT, col_off:col_off + NLON, :].reshape(-1, CIN)
            tap_parts.append(jnp.dot(act_tap.T, up_flat, preferred_element_type=jnp.float32))
        grad_total = grad_total + jnp.stack(tap_parts, axis=1)
        return (grad_total, data_sum.reshape(NLAT, NLON, CIN).astype(jnp.bfloat16))
    grad_total, input_grad = lax.scan(one_sample, jnp.zeros((CIN, 9, COUT), jnp.float32), (activations, upstream))
    max_norm = math.sqrt(float(CIN * TAPS * COUT))
    square_sum = jnp.sum(grad_total * grad_total)
    clip_factor = jnp.minimum(1.0, max_norm / (jnp.sqrt(square_sum) + norm_eps))
    grad_scaled = clip_factor * grad_total
    new_one = beta_one * moment_one + (1.0 - beta_one) * grad_scaled
    new_two = beta_two * moment_two + (1.0 - beta_two) * grad_scaled * grad_scaled
    first_hat = new_one / (1.0 - beta_one ** step_count)
    second_hat = new_two / (1.0 - beta_two ** step_count)
    new_master = master - learn_rate * (first_hat / (jnp.sqrt(second_hat) + adam_eps) + decay_rate * master)
    new_weights = new_master.astype(jnp.bfloat16)
    return (input_grad, new_weights, new_master, new_one, new_two, grad_scaled)
```

```python
import functools
import math

import jax
import jax.numpy as jnp
from jax import lax
from jax.experimental import pallas as pl
from jax.experimental.pallas import tpu as pltpu
from jax.sharding import PartitionSpec as P

CIN = 512
COUT = 512
TAPS = 9

learn_rate = 0.01
beta_one = 0.9
beta_two = 0.999
adam_eps = 1e-08
decay_rate = 0.1
step_count = 10.0
norm_eps = 1e-06

F32 = jnp.float32
BF16 = jnp.bfloat16
MESH = pl.DeviceIdType.MESH

HALO = 0
PAIR = HALO + 8
RS_A = PAIR + 3
RS_Z = RS_A + 9
RS_F = RS_Z + 21
NORM = RS_F + 21
GATHER = NORM + 30
GATHER_SIZE = 7 + 7 + 24 + 4
SLOTS = GATHER + 2 * GATHER_SIZE

ROW_ORDER = (1, 0, 2)


def nt_dot(a, b):
    return lax.dot_general(a, b, (((1,), (1,)), ((), ())), preferred_element_type=F32)


def nn_dot(a, b):
    return lax.dot_general(a, b, (((1,), (0,)), ((), ())), preferred_element_type=F32)


def ordered(channel, color):
    r = channel & 1
    core = (channel >> 1) & 1
    x = ((channel >> 2) & 1) * 2 + ((channel >> 8) & 1)
    z = (channel >> 3) & 7
    y = (channel >> 6) & 3
    first = y * (1 - color) + x * color
    last = x * (1 - color) + y * color
    return first * 128 + z * 16 + core * 8 + last * 2 + r


def kernel(
    act, up, master, one, two,
    out_in, out_w, out_master, out_one, out_two, out_grad,
    u, at_m, at_o, perm_m, perm_o, edge_f, edge, edge_in,
    g_m, g_o, g_l, b1, l1, t1, b2, l2, fo, fl, grad, nb, nl,
    wf, wl, wt, wg_m, wg_o, wn, prod, local, ss, rs,
):
    lat = lax.axis_index("lat")
    lon = lax.axis_index("lon")
    x_lo, y = lat // 4, lat % 4
    z, x_hi, core = lon // 4, (lon // 2) % 2, lon % 2
    x = x_hi * 2 + x_lo

    def device(x_, y_, z_, core_):
        return ((x_ % 2) * 4 + y_, z_ * 4 + (x_ // 2) * 2 + core_)

    def along(color, step, core_):
        return device((x + step * color) % 4, (y + step * (1 - color)) % 4, z, core_)

    def z_peer(d):
        return device(x, y, (z + d) % 8, core)

    sibling = device(x, y, z, 1 - core)
    first_me = y * (1 - core) + x * core
    last_me = x * (1 - core) + y * core
    other = 1 - core

    def remote(src, dst, slot, where):
        return pltpu.make_async_remote_copy(
            src_ref=src, dst_ref=dst, send_sem=ss.at[slot], recv_sem=rs.at[slot],
            device_id=where, device_id_type=MESH,
        )

    sent = []

    def send(src, dst, slot, where):
        copy = remote(src, dst, slot, where)
        copy.start()
        sent.append(copy)

    def received(dst, slot):
        remote(dst, dst, slot, sibling).wait_recv()

    lanes_m = pl.ds(pl.multiple_of(core * 256, 256), 256)
    lanes_o = pl.ds(pl.multiple_of(other * 256, 256), 256)

    lat_down, lat_up = (lat + 1) % 8, (lat + 7) % 8
    lon_right, lon_left = (lon + 1) % 32, (lon + 31) % 32
    halo_peers = [
        (lat_down, lon), (lat_up, lon),
        (lat, lon_right), (lat_down, lon_right), (lat_up, lon_right),
        (lat, lon_left), (lat_down, lon_left), (lat_up, lon_left),
    ]
    plane_peers = [device((x + d // 4) % 4, (y + d % 4) % 4, z, core) for d in range(1, 16)]
    line_peers = [device(x, y, (z + d // 2) % 8, (core + d % 2) % 2) for d in range(1, 16)]
    cross_peers = [along(color, step, other) for color in (0, 1) for step in (1, 2, 3)]
    peers = halo_peers + plane_peers + line_peers + cross_peers
    barrier = pltpu.get_barrier_semaphore()
    for peer in peers:
        pl.semaphore_signal(barrier, inc=1, device_id=peer, device_id_type=MESH)

    load = pltpu.make_async_copy(up, u.at[pl.ds(1, 4)], local.at[0])
    load.start()

    rows = lax.broadcasted_iota(jnp.int32, (512, 512), 0)
    cols = lax.broadcasted_iota(jnp.int32, (512, 512), 1)

    def one_hot(mask):
        return jnp.where(mask, 1.0, 0.0).astype(BF16)

    act_all = act[...].reshape(1536, 512)
    for color, at in ((core, at_m), (other, at_o)):
        pick = one_hot(rows == ordered(cols, color))
        at[0] = nt_dot(pick, act_all).astype(BF16)
    perm_m[...] = one_hot(ordered(rows, core) == cols)
    perm_o[...] = one_hot(ordered(rows, other) == cols)

    load.wait()
    for i in range(4):
        for b in range(4):
            g = i * 4 + b
            edge_f[0, g : g + 1, :] = u[1 + i, b, 0:16, :].astype(F32)[1:2]
            edge_f[1, g : g + 1, :] = u[1 + i, b, 80:96, :].astype(F32)[10:11]
    edge[...] = edge_f[...].astype(BF16)
    wf[0] = master[:, :, 0:256]
    wf[1] = master[:, :, 256:512]

    pl.semaphore_wait(barrier, len(peers))

    for k, where in enumerate(halo_peers[2:5]):
        send(edge.at[1], edge_in.at[0, k], HALO + 2 + k, where)
    for k, where in enumerate(halo_peers[5:8]):
        send(edge.at[0], edge_in.at[1, k], HALO + 5 + k, where)
    send(up.at[3], u.at[0], HALO + 0, halo_peers[0])
    send(up.at[0], u.at[5], HALO + 1, halo_peers[1])

    def gather_start(which):
        base = GATHER + which * GATHER_SIZE
        for dd in range(1, 8):
            da, dc = dd % 4, dd // 4
            color = core if dc == 0 else other
            here = x * (1 - color) + y * color
            send(
                wf.at[color], wl.at[which, core, here], base + dd - 1,
                along(1 - color, da, color),
            )
        wl[which, core, last_me] = wf[core]

    def gather_z(which):
        base = GATHER + which * GATHER_SIZE
        for dd in range(1, 8):
            received(wl.at[which, 0, 0], base + dd - 1)
        for c in range(2):
            for a in range(4):
                row = c * 8 + a * 2
                wt[:, row : row + 2, :] = wl[which, c, a]
        wg_m[which, first_me, z] = wt[...].astype(BF16)
        mine = wg_m.at[which, first_me, z]
        for d in range(1, 8):
            send(mine, mine, base + 7 + d - 1, z_peer(d))
        for a in range(1, 4):
            send(mine, mine, base + 14 + a - 1, along(core, a, core))

    def gather_first(which):
        base = GATHER + which * GATHER_SIZE
        for d in (1, 7, 2, 6, 3, 5, 4):
            block = wg_m.at[which, first_me, (z + 8 - d) % 8]
            received(block, base + 7 + d - 1)
            for a in range(1, 4):
                send(block, block, base + 14 + d * 3 + a - 1, along(core, a, core))
        block = wg_m.at[which, first_me]
        send(block, wg_o.at[which, first_me], base + 38, sibling)

    def gather_pair(which):
        base = GATHER + which * GATHER_SIZE
        for a in (1, 3, 2):
            place = (first_me + 4 - a) % 4
            for d in range(8):
                received(wg_m.at[which, 0, 0], base + 14 + d * 3 + a - 1)
            block = wg_m.at[which, place]
            send(block, wg_o.at[which, place], base + 38 + a, sibling)

    def gather_end(which):
        base = GATHER + which * GATHER_SIZE
        for a in range(4):
            received(wg_o.at[which, 0], base + 38 + a)

    def natural(which, dst):
        @pl.loop(0, 9)
        def _(tap):
            got = wg_m[which, :, :, tap].reshape(512, 256)
            dst[tap, :, lanes_m] = nn_dot(perm_m[...], got).astype(BF16)
            got = wg_o[which, :, :, tap].reshape(512, 256)
            dst[tap, :, lanes_o] = nn_dot(perm_o[...], got).astype(BF16)

    gather_start(0)

    for at in (at_m, at_o):
        base_at = at[0]
        at[1] = pltpu.roll(base_at, 1, 1)
        at[2] = pltpu.roll(base_at, 2, 1)

    def put_row(i, b, start, row, value):
        tile = u[i, b, start : start + 16, :].astype(F32)
        ids = lax.broadcasted_iota(jnp.int32, (16, 512), 0)
        u[i, b, start : start + 16, :] = jnp.where(ids == row, value, tile).astype(BF16)

    for k in range(6):
        received(edge_in.at[0, 0], HALO + 2 + k)
    for side, (start, row) in enumerate(((0, 0), (80, 11))):
        got = edge_in[side, 0].astype(F32)
        for i in range(4):
            for b in range(4):
                g = i * 4 + b
                put_row(1 + i, b, start, row, got[g : g + 1])

    def terms(g):
        r = ROW_ORDER[g]
        lo = 2 - r

        @pl.loop(0, 3)
        def _(s):
            field = u[lo : lo + 4, :, :, lanes_o].reshape(1536, 256)
            g_o[g, s] = nn_dot(at_o[2 - s], field)

        send(g_o.at[g], g_l.at[g], PAIR + g, sibling)

        @pl.loop(0, 3)
        def _(s):
            field = u[lo : lo + 4, :, :, lanes_m].reshape(1536, 256)
            g_m[g, s] = nn_dot(at_m[2 - s], field)

    def reduce_first(g):
        received(g_l.at[g], PAIR + g)

        @pl.loop(0, 4)
        def _(a):
            block = pl.ds(pl.multiple_of(a * 128, 128), 128)
            total = g_m[g, :, block, :] + g_l[g, :, block, :]
            g_m[g, :, block, :] = total
            b1[g, a] = total.astype(BF16)

        for a in range(1, 4):
            send(
                b1.at[g, (first_me + a) % 4], l1.at[g, a - 1],
                RS_A + g * 3 + a - 1, along(core, a, core),
            )

    def reduce_z(g):
        for a in range(1, 4):
            received(l1.at[g, a - 1], RS_A + g * 3 + a - 1)
        block = pl.ds(pl.multiple_of(first_me * 128, 128), 128)
        total = g_m[g, :, block, :]
        for a in range(3):
            total = total + l1[g, a].astype(F32)
        for k in range(8):
            part = total[:, k * 16 : (k + 1) * 16, :]
            t1[g, k] = part
            b2[g, k] = part.astype(BF16)
        for d in range(1, 8):
            send(b2.at[g, (z + d) % 8], l2.at[g, d - 1], RS_Z + g * 7 + d - 1, z_peer(d))

    def reduce_last(g):
        for d in range(1, 8):
            received(l2.at[g, d - 1], RS_Z + g * 7 + d - 1)
        total = t1[g, z]
        for d in range(7):
            total = total + l2[g, d].astype(F32)
        for c in range(2):
            for a in range(4):
                row = c * 8 + a * 2
                fo[g, c, a] = total[:, row : row + 2, :]
        fl[g, 0] = fo[g, core, last_me]
        for dd in range(1, 8):
            da, dc = dd % 4, dd // 4
            core_to = core if dc == 0 else other
            send(
                fo.at[g, core_to, (last_me + da) % 4], fl.at[g, dd],
                RS_F + g * 7 + dd - 1, along(other, da, core_to),
            )

    def finish(g):
        r = ROW_ORDER[g]
        for dd in range(1, 8):
            received(fl.at[g, dd], RS_F + g * 7 + dd - 1)
        grad[3 * r : 3 * r + 3, :, lanes_m] = (fl[g, 0] + fl[g, 1]) + (fl[g, 2] + fl[g, 3])
        grad[3 * r : 3 * r + 3, :, lanes_o] = (fl[g, 4] + fl[g, 5]) + (fl[g, 6] + fl[g, 7])

    def input_part(i):
        for s in range(3):
            total = nt_dot(u[i + 2].reshape(384, 512), wn[s])
            total = total + nt_dot(u[i + 1].reshape(384, 512), wn[3 + s])
            total = total + nt_dot(u[i].reshape(384, 512), wn[6 + s])
            prod[s, :, 0:96, :] = total.reshape(4, 96, 512)
        for b in range(4):
            out_in[i, b] = (
                prod[2, b, 0:96, :] + prod[1, b, 1:97, :] + prod[0, b, 2:98, :]
            ).astype(BF16)

    terms(0)
    gather_z(0)

    received(u.at[0], HALO + 0)
    received(u.at[5], HALO + 1)

    @pl.when(lat == 0)
    def _():
        u[0] = jnp.zeros((4, 96, 512), BF16)

    @pl.when(lat == 7)
    def _():
        u[5] = jnp.zeros((4, 96, 512), BF16)

    low = jnp.where(lat == 0, 0.0, 1.0)
    high = jnp.where(lat == 7, 0.0, 1.0)
    for side, (start, row) in enumerate(((0, 0), (80, 11))):
        above = edge_in[side, 1].astype(F32) * low
        below = edge_in[side, 2].astype(F32) * high
        for b in range(4):
            put_row(0, b, start, row, above[12 + b : 13 + b])
            put_row(5, b, start, row, below[b : b + 1])

    reduce_first(0)
    terms(1)
    gather_first(0)
    reduce_first(1)
    terms(2)
    reduce_z(0)
    reduce_first(2)
    gather_pair(0)
    reduce_z(1)
    reduce_last(0)
    reduce_z(2)
    gather_end(0)
    natural(0, wn)
    reduce_last(1)
    reduce_last(2)
    prod[:, :, 96:104, :] = jnp.zeros((3, 4, 8, 512), F32)
    finish(0)
    finish(1)
    finish(2)

    g_sum = grad[...]
    nb[0] = jnp.zeros((8, 128), F32) + jnp.sum(g_sum * g_sum)
    for d in range(1, 16):
        send(nb.at[0], nl.at[0, d], NORM + d - 1, plane_peers[d - 1])
    nl[0, 0] = nb[0]
    input_part(0)
    for d in range(1, 16):
        received(nl.at[0, d], NORM + d - 1)
    plane_sum = jnp.sum(nl[0], axis=0)
    nb[1] = plane_sum
    for d in range(1, 16):
        send(nb.at[1], nl.at[1, d], NORM + 15 + d - 1, line_peers[d - 1])
    nl[1, 0] = plane_sum
    input_part(1)
    for d in range(1, 16):
        received(nl.at[1, d], NORM + 15 + d - 1)
    square_sum = jnp.max(jnp.sum(nl[1], axis=0), axis=(0, 1), keepdims=True)
    max_norm = math.sqrt(float(CIN * TAPS * COUT))
    clip = jnp.minimum(1.0, max_norm / (jnp.sqrt(square_sum) + norm_eps))
    scaled = g_sum * clip.reshape(1, 1, 1)
    old = master[...]
    new_one = beta_one * one[...] + (1.0 - beta_one) * scaled
    new_two = beta_two * two[...] + (1.0 - beta_two) * scaled * scaled
    first_hat = new_one / (1.0 - beta_one**step_count)
    second_hat = new_two / (1.0 - beta_two**step_count)
    new_master = old - learn_rate * (
        first_hat / (jnp.sqrt(second_hat) + adam_eps) + decay_rate * old
    )
    for copy in sent:
        copy.wait_send()
    sent.clear()
    wf[0] = new_master[:, :, 0:256]
    wf[1] = new_master[:, :, 256:512]
    gather_start(1)
    out_master[...] = new_master
    out_one[...] = new_one
    out_two[...] = new_two
    out_grad[...] = scaled
    input_part(2)
    gather_z(1)
    input_part(3)
    gather_first(1)
    gather_pair(1)
    gather_end(1)
    natural(1, out_w)
    for copy in sent:
        copy.wait_send()


def per_device(activations, upstream, master, moment_one, moment_two):
    def laid(field, before):
        field = jnp.transpose(field, (1, 0, 2, 3))
        return jnp.pad(field, ((0, 0), (0, 0), (before, 6 - before), (0, 0)))

    act = laid(activations, 0)
    up = laid(upstream, 1)
    state = [jnp.transpose(v, (1, 0, 2)) for v in (master, moment_one, moment_two)]
    vmem = pl.BlockSpec(memory_space=pltpu.VMEM)
    shard = jax.ShapeDtypeStruct((9, 2, 512), F32)
    outs = pl.pallas_call(
        kernel,
        out_shape=(
            jax.ShapeDtypeStruct((4, 4, 96, 512), BF16),
            jax.ShapeDtypeStruct((9, 512, 512), BF16),
            shard, shard, shard, shard,
        ),
        in_specs=[vmem, pl.BlockSpec(memory_space=pl.ANY), vmem, vmem, vmem],
        out_specs=(vmem,) * 6,
        scratch_shapes=[
            pltpu.VMEM((6, 4, 96, 512), BF16),
            pltpu.VMEM((3, 512, 1536), BF16),
            pltpu.VMEM((3, 512, 1536), BF16),
            pltpu.VMEM((512, 512), BF16),
            pltpu.VMEM((512, 512), BF16),
            pltpu.VMEM((2, 16, 512), F32),
            pltpu.VMEM((2, 16, 512), BF16),
            pltpu.VMEM((2, 3, 16, 512), BF16),
            pltpu.VMEM((3, 3, 512, 256), F32),
            pltpu.VMEM((3, 3, 512, 256), F32),
            pltpu.VMEM((3, 3, 512, 256), F32),
            pltpu.VMEM((3, 4, 3, 128, 256), BF16),
            pltpu.VMEM((3, 3, 3, 128, 256), BF16),
            pltpu.VMEM((3, 8, 3, 16, 256), F32),
            pltpu.VMEM((3, 8, 3, 16, 256), BF16),
            pltpu.VMEM((3, 7, 3, 16, 256), BF16),
            pltpu.VMEM((3, 2, 4, 3, 2, 256), F32),
            pltpu.VMEM((3, 8, 3, 2, 256), F32),
            pltpu.VMEM((9, 2, 512), F32),
            pltpu.VMEM((2, 8, 128), F32),
            pltpu.VMEM((2, 16, 8, 128), F32),
            pltpu.VMEM((2, 9, 2, 256), F32),
            pltpu.VMEM((2, 2, 4, 9, 2, 256), F32),
            pltpu.VMEM((9, 16, 256), F32),
            pltpu.VMEM((2, 4, 8, 9, 16, 256), BF16),
            pltpu.VMEM((2, 4, 8, 9, 16, 256), BF16),
            pltpu.VMEM((9, 512, 512), BF16),
            pltpu.VMEM((3, 4, 104, 512), F32),
            pltpu.SemaphoreType.DMA((1,)),
            pltpu.SemaphoreType.DMA((SLOTS,)),
            pltpu.SemaphoreType.DMA((SLOTS,)),
        ],
        compiler_params=pltpu.CompilerParams(
            collective_id=0, has_side_effects=True, vmem_limit_bytes=63 * 1024 * 1024
        ),
        name="conv_step",
    )(act, up, *state)
    input_grad = jnp.transpose(outs[0][:, :, :90, :], (1, 0, 2, 3))
    rest = [jnp.transpose(v, (1, 0, 2)) for v in outs[1:]]
    return (input_grad, *rest)


def solution(mesh):
    field = P(None, "lat", "lon", None)
    state = P(("lat", "lon"), None, None)
    return jax.shard_map(
        per_device,
        mesh=mesh,
        in_specs=(field, field, state, state, state),
        out_specs=(field, P(), state, state, state, state),
        check_vma=False,
    )
```

```python
import functools
import math

import jax
import jax.numpy as jnp
from jax import lax
from jax.experimental import pallas as pl
from jax.experimental.pallas import tpu as pltpu
from jax.sharding import PartitionSpec as P

CIN = 512
COUT = 512
TAPS = 9

learn_rate = 0.01
beta_one = 0.9
beta_two = 0.999
adam_eps = 1e-08
decay_rate = 0.1
step_count = 10.0
norm_eps = 1e-06

F32 = jnp.float32
BF16 = jnp.bfloat16
MESH = pl.DeviceIdType.MESH

R_EDGE, R_SLAB, R_PAIR, R_A, R_Z, R_F, R_N = 0, 1, 3, 6, 18, 21, 24
R_LAST, R_GZ, R_NEAR, R_FAR, R_GP, R_SLOTS = 26, 27, 35, 51, 67, 68
S_EDGE, S_SLAB, S_PAIR, S_AH, S_AU, S_Z, S_F, S_N = 0, 1, 2, 5, 8, 11, 14, 17
S_LAST, S_GZ, S_NEAR, S_FAR, S_GP, S_SLOTS = 19, 20, 21, 22, 23, 24

ROW_ORDER = (1, 0, 2)


def nt_dot(a, b):
    return lax.dot_general(a, b, (((1,), (1,)), ((), ())), preferred_element_type=F32)


def nn_dot(a, b):
    return lax.dot_general(a, b, (((1,), (0,)), ((), ())), preferred_element_type=F32)


def ordered(channel, color):
    r = channel & 1
    core = (channel >> 1) & 1
    x = ((channel >> 2) & 1) * 2 + ((channel >> 8) & 1)
    z = (channel >> 3) & 7
    y = (channel >> 6) & 3
    first = y * (1 - color) + x * color
    last = x * (1 - color) + y * color
    return first * 128 + z * 16 + core * 8 + last * 2 + r


def block_order(place, color):
    r = place & 1
    last = (place >> 1) & 3
    core = (place >> 3) & 1
    z = (place >> 4) & 7
    high = place >> 7
    y_way = (last & 1) * 128 + high * 64 + z * 8 + (last >> 1) * 4 + core * 2 + r
    x_way = last * 64 + z * 8 + high * 4 + core * 2 + r
    return y_way * (1 - color) + x_way * color


def one_hot(mask):
    return jnp.where(mask, 1.0, 0.0).astype(BF16)


def make_perms(perm, core):
    rows = lax.broadcasted_iota(jnp.int32, (256, 256), 0)
    cols = lax.broadcasted_iota(jnp.int32, (1, 256), 1)
    perm[0] = one_hot(rows == block_order(cols, core))
    perm[1] = one_hot(rows == block_order(cols, 1 - core))


def natural(perm, w_m, w_o, dst, core, tap):
    for k, (w, color) in enumerate(((w_m, core), (w_o, 1 - core))):
        lanes = pl.ds(pl.multiple_of(color * 256, 256), 256)
        for parity in (0, 1):
            low = w[parity, :, tap].reshape(128, 256)
            high = w[parity + 2, :, tap].reshape(128, 256)
            got = jnp.concatenate([low, high], axis=0)
            block = nn_dot(perm[k], got).astype(BF16)
            for q in range(4):
                y_way = (q // 2) * 256 + (q % 2) * 128 + parity * 64
                x_way = parity * 256 + q * 64
                start = pl.multiple_of(y_way * (1 - color) + x_way * color, 64)
                dst[tap, pl.ds(start, 64), lanes] = block[q * 64 : (q + 1) * 64]


def finish_kernel(
    w_m, w_o, v0, v1, v2, v3, out_w, o0, o1, o2, o3, wn, perm, local
):
    core = lax.axis_index("lon") % 2
    copies = [
        pltpu.make_async_copy(v, o, local.at[k])
        for k, (v, o) in enumerate(((v0, o0), (v1, o1), (v2, o2), (v3, o3)))
    ]
    for copy in copies:
        copy.start()
    make_perms(perm, core)

    @pl.loop(0, 9)
    def _(tap):
        natural(perm, w_m, w_o, wn, core, tap)
        pltpu.make_async_copy(wn.at[tap], out_w.at[tap], local.at[4 + tap]).start()

    for copy in copies:
        copy.wait()
    for tap in range(9):
        pltpu.make_async_copy(wn.at[tap], out_w.at[tap], local.at[4 + tap]).wait()


def kernel(
    act, up, master, one_far, two_far,
    oi, new_m, new_o, out_master, out_one, out_two, out_grad,
    one, two, u, ap, at_m, at_o, perm, edge_f, edge, edge_in, hal,
    g_m, g_o, g_l, bh, lh, bu, lu, t1, b2, l2, fo, fl, grad, nb, nl,
    wf, wl, wt, old_m, old_o, wn, prod, local, ss, rs,
):
    lat = lax.axis_index("lat")
    lon = lax.axis_index("lon")
    x_lo, y = lat // 4, lat % 4
    z, x_hi, core = lon // 4, (lon // 2) % 2, lon % 2
    x = x_hi * 2 + x_lo

    def device(x_, y_, z_, core_):
        return ((x_ % 2) * 4 + y_, z_ * 4 + (x_ // 2) * 2 + core_)

    def along(color, step, core_):
        return device((x + step * color) % 4, (y + step * (1 - color)) % 4, z, core_)

    def z_peer(d):
        return device(x, y, (z + d) % 8, core)

    other = 1 - core
    sibling = device(x, y, z, other)
    after, before = along(core, 1, core), along(core, 3, core)
    first_me = y * (1 - core) + x * core
    last_me = x * (1 - core) + y * core

    def remote(src, dst, out_slot, in_slot, where):
        return pltpu.make_async_remote_copy(
            src_ref=src, dst_ref=dst, send_sem=ss.at[out_slot], recv_sem=rs.at[in_slot],
            device_id=where, device_id_type=MESH,
        )

    def send(src, dst, out_slot, in_slot, where):
        remote(src, dst, out_slot, in_slot, where).start()

    def received(dst, slot):
        remote(dst, dst, 0, slot, sibling).wait_recv()

    def left(src, slot):
        remote(src, src, slot, 0, sibling).wait_send()

    lanes_m = pl.ds(pl.multiple_of(core * 256, 256), 256)
    lanes_o = pl.ds(pl.multiple_of(other * 256, 256), 256)

    lat_down, lat_up = (lat + 1) % 8, (lat + 7) % 8
    lon_right, lon_left = (lon + 1) % 32, (lon + 31) % 32
    halo_peers = [
        (lat_down, lon), (lat_up, lon),
        (lat, lon_right), (lat_down, lon_right), (lat_up, lon_right),
        (lat, lon_left), (lat_down, lon_left), (lat_up, lon_left),
    ]
    plane_peers = [device((x + d // 4) % 4, (y + d % 4) % 4, z, core) for d in range(1, 16)]
    line_peers = [device(x, y, (z + d // 2) % 8, (core + d % 2) % 2) for d in range(1, 16)]
    cross_peers = [along(color, step, other) for color in (0, 1) for step in (1, 2, 3)]
    peers = halo_peers + plane_peers + line_peers + cross_peers
    barrier = pltpu.get_barrier_semaphore()
    for peer in peers:
        pl.semaphore_signal(barrier, inc=1, device_id=peer, device_id_type=MESH)

    loads = [
        pltpu.make_async_copy(src, dst, local.at[k])
        for k, (src, dst) in enumerate(
            ((one_far, one), (two_far, two))
        )
    ]
    for copy in loads:
        copy.start()
    wg_m, wg_o = (old_m, new_m), (old_o, new_o)
    wf[0] = master[:, :, 0:256]
    wf[1] = master[:, :, 256:512]
    for i in range(4):
        for b in range(4):
            g = i * 4 + b
            edge_f[0, g : g + 1, :] = up[i, b, 0:16, :].astype(F32)[0:1]
            edge_f[1, g : g + 1, :] = up[i, b, 80:90, :].astype(F32)[9:10]
    edge[...] = edge_f[...].astype(BF16)

    with jax.named_scope("barrier"):
        pl.semaphore_wait(barrier, len(peers))

    def gather_start(which):
        for dd in range(1, 8):
            da, dc = dd % 4, dd // 4
            color = core if dc == 0 else other
            here = x * (1 - color) + y * color
            send(
                wf.at[color], wl.at[which, core * 4 + here], S_LAST, R_LAST,
                along(1 - color, da, color),
            )
        wl[which, core * 4 + last_me] = wf[core]

    def piece(which, e, step=0):
        return wg_m[which].at[(first_me + 4 + step) % 4, (z + 8 + e) % 8]

    low_half, high_half = pl.ds(0, 128), pl.ds(128, 128)

    def to_pair(which, e, step):
        there = wg_o[which].at[(first_me + 4 + step) % 4, (z + 8 + e) % 8]
        send(piece(which, e, step), there, S_GP, R_GP, sibling)

    def gather_near(which, e):
        block = piece(which, e)
        send(block, block, S_NEAR, R_NEAR + 2 * (e % 8), after)
        send(block, block, S_NEAR, R_NEAR + 2 * (e % 8) + 1, before)
        to_pair(which, e, 0)

    def gather_z(which):
        received(wl.at[which, pl.ds(0, 7)], R_LAST)
        for k in range(8):
            wt[:, k * 2 : k * 2 + 2, :] = wl[which, k]
        wg_m[which][first_me, z] = wt[...].astype(BF16)
        mine = piece(which, 0)
        for k, d in enumerate((1, 7, 2, 6)):
            send(mine, mine, S_GZ, R_GZ + k, z_peer(d))
        gather_near(which, 0)

    def gather_z1(which):
        for k, e in enumerate((-1, 1)):
            received(piece(which, e), R_GZ + k)
            gather_near(which, e)

    def gather_z2(which):
        for k, e in enumerate((-2, 2)):
            block = piece(which, e)
            received(block, R_GZ + 2 + k)
            send(block, block, S_GZ, R_GZ + 4 + k, z_peer(1 if e < 0 else 7))
            gather_near(which, e)

    def gather_z3(which):
        for k, (e, half) in enumerate(((-3, low_half), (3, high_half))):
            block = piece(which, e)
            received(block, R_GZ + 4 + k)
            part = block.at[:, :, half]
            send(part, part, S_GZ, R_GZ + 6 + k, z_peer(1 if e < 0 else 7))
            gather_near(which, e)

    def gather_z4(which):
        block = piece(which, 4)
        received(block.at[:, :, low_half], R_GZ + 6)
        received(block.at[:, :, high_half], R_GZ + 7)
        gather_near(which, 4)

    def gather_far(which, *places):
        for e in places:
            for k, (step, half, where) in enumerate(
                ((-1, low_half, after), (1, high_half, before))
            ):
                block = piece(which, e, step)
                received(block, R_NEAR + 2 * (e % 8) + k)
                part = block.at[:, :, half]
                send(part, part, S_FAR, R_FAR + 2 * (e % 8) + k, where)
                to_pair(which, e, step)

    def gather_last(which, *places):
        for e in places:
            block = piece(which, e, 2)
            received(block.at[:, :, low_half], R_FAR + 2 * (e % 8))
            received(block.at[:, :, high_half], R_FAR + 2 * (e % 8) + 1)
            to_pair(which, e, 2)

    def gather_end(which):
        received(wg_o[which], R_GP)

    def gather_left(which):
        w = wg_m[which]
        left(wl.at[which, pl.ds(0, 7)], S_LAST)
        left(w.at[0, pl.ds(0, 7)], S_GZ)
        left(w.at[pl.ds(0, 2)], S_NEAR)
        left(w.at[0], S_FAR)
        left(w, S_GP)

    gather_start(0)

    for k, where in enumerate(halo_peers[2:5]):
        send(edge.at[1], edge_in.at[0, k], S_EDGE, R_EDGE, where)
    for k, where in enumerate(halo_peers[5:8]):
        send(edge.at[0], edge_in.at[1, k], S_EDGE, R_EDGE, where)
    send(up.at[3], hal.at[0], S_SLAB, R_SLAB, halo_peers[0])
    send(up.at[0], hal.at[1], S_SLAB, R_SLAB + 1, halo_peers[1])

    ap[:, :, 80:96, :] = jnp.zeros((4, 4, 16, 512), BF16)
    ap[:, :, 0:90, :] = act[...]
    u[:, :, 80:96, :] = jnp.zeros((6, 4, 16, 512), BF16)
    u[1:5, :, 0:90, :] = up[...]
    rows = lax.broadcasted_iota(jnp.int32, (512, 512), 0)
    cols = lax.broadcasted_iota(jnp.int32, (1, 512), 1)
    group_end = lax.broadcasted_iota(jnp.int32, (512, 1536), 1) % 96 == 95
    act_all = ap[...].reshape(1536, 512)
    for color, at in ((other, at_o), (core, at_m)):
        pick = one_hot(rows == ordered(cols, color))
        base_at = nt_dot(pick, act_all)
        half_at = base_at.astype(BF16)
        at[1] = half_at
        at[0] = pltpu.roll(half_at, 1, 1)
        at[2] = jnp.where(group_end, pltpu.roll(half_at, 95, 1), pltpu.roll(half_at, 1535, 1))

    def put_edges(i, b, left, right):
        tile = u[i, b, 80:96, :].astype(F32)
        ids = lax.broadcasted_iota(jnp.int32, (16, 512), 0)
        tile = jnp.where(ids == 10, right, jnp.where(ids == 15, left, tile))
        u[i, b, 80:96, :] = tile.astype(BF16)

    with jax.named_scope("gz_old"):
        gather_z(0)
    with jax.named_scope("edges"):
        received(edge_in, R_EDGE)
        west, east = edge_in[0, 0].astype(F32), edge_in[1, 0].astype(F32)
        for i in range(4):
            for b in range(4):
                g = i * 4 + b
                put_edges(1 + i, b, west[g : g + 1], east[g : g + 1])

    def product(g, rows, cols, add):
        def both(at, dst, lanes):
            @pl.loop(0, 3)
            def _(s):
                field = u[rows, :, :, lanes].reshape(-1, 256)
                term = nn_dot(at[s, :, cols], field)
                dst[s] = dst[s] + term if add else term

        both(at_o, g_o.at[g], lanes_o)
        if add or g == 0:
            send(g_o.at[g], g_l.at[g], S_PAIR + g, R_PAIR + g, sibling)
        both(at_m, g_m.at[g], lanes_m)

    def rows_of(step):
        return pl.ds(pl.multiple_of(((first_me + step) % 4) * 128, 128), 128)

    def reduce_far(g):
        received(g_l.at[g], R_PAIR + g)
        total = g_m[g, :, rows_of(2), :] + g_l[g, :, rows_of(2), :]
        bh[g, 0] = total[:, 0:64].astype(BF16)
        bh[g, 1] = total[:, 64:128].astype(BF16)
        send(bh.at[g, 0], lh.at[g, 0], S_AH + g, R_A + g * 4, after)
        send(bh.at[g, 1], lh.at[g, 1], S_AH + g, R_A + g * 4 + 1, before)

    def reduce_near(g):
        for k, (step, where) in enumerate(((1, after), (3, before))):
            total = g_m[g, :, rows_of(step), :] + g_l[g, :, rows_of(step), :]
            received(lh.at[g, k], R_A + g * 4 + k)
            came = lh[g, k].astype(F32)
            part = total[:, k * 64 : (k + 1) * 64] + came
            rest = total[:, (1 - k) * 64 : (2 - k) * 64]
            bu[g, k, :, k * 64 : (k + 1) * 64, :] = part.astype(BF16)
            bu[g, k, :, (1 - k) * 64 : (2 - k) * 64, :] = rest.astype(BF16)
            send(bu.at[g, k], lu.at[g, k], S_AU + g, R_A + g * 4 + 2 + k, where)

    def reduce_z(g):
        total = g_m[g, :, rows_of(0), :] + g_l[g, :, rows_of(0), :]
        for k in range(2):
            received(lu.at[g, k], R_A + g * 4 + 2 + k)
            total = total + lu[g, k].astype(F32)
        for k in range(8):
            part = total[:, k * 16 : (k + 1) * 16, :]
            t1[g, k] = part
            b2[g, k] = part.astype(BF16)
        for d in (4, 3, 5, 2, 6, 1, 7):
            send(b2.at[g, (z + d) % 8], l2.at[g, d - 1], S_Z + g, R_Z + g, z_peer(d))

    def reduce_last(g):
        received(l2.at[g], R_Z + g)
        total = t1[g, z]
        for d in range(7):
            total = total + l2[g, d].astype(F32)
        for c in range(2):
            for a in range(4):
                row = c * 8 + a * 2
                fo[g, c, a] = total[:, row : row + 2, :]
        fl[g, 0] = fo[g, core, last_me]
        for dd in range(1, 8):
            da, dc = dd % 4, dd // 4
            core_to = core if dc == 0 else other
            send(
                fo.at[g, core_to, (last_me + da) % 4], fl.at[g, dd],
                S_F + g, R_F + g, along(other, da, core_to),
            )

    def finish(g):
        r = ROW_ORDER[g]
        received(fl.at[g, pl.ds(1, 7)], R_F + g)
        grad[3 * r : 3 * r + 3, :, lanes_m] = (fl[g, 0] + fl[g, 1]) + (fl[g, 2] + fl[g, 3])
        grad[3 * r : 3 * r + 3, :, lanes_o] = (fl[g, 4] + fl[g, 5]) + (fl[g, 6] + fl[g, 7])

    def input_part(i):
        for s in range(3):
            total = nt_dot(u[i + 2].reshape(384, 512), wn[s])
            total = total + nt_dot(u[i + 1].reshape(384, 512), wn[3 + s])
            total = total + nt_dot(u[i].reshape(384, 512), wn[6 + s])
            total = total.reshape(4, 96, 512)
            if s == 2:
                prod[2, :, 8:104, :] = total
                prod[2, :, 7:8, :] = total[:, 95:96, :]
            else:
                prod[s, :, 0:96, :] = total
        for b in range(4):
            whole = prod[0, b, 1:97, :] + prod[1, b, 0:96, :] + prod[2, b, 7:103, :]
            oi[i, b] = whole[0:90].astype(BF16)

    with jax.named_scope("terms0"):
        product(0, pl.ds(1, 4), pl.ds(0, 1536), False)
    with jax.named_scope("gz1_old"):
        gather_z1(0)
    with jax.named_scope("rf0"):
        reduce_far(0)
    with jax.named_scope("own1"):
        product(1, pl.ds(2, 3), pl.ds(0, 1152), False)
    with jax.named_scope("rn0"):
        reduce_near(0)
    with jax.named_scope("gz2_old"):
        gather_z2(0)
        gather_far(0, 0)
    with jax.named_scope("own2"):
        product(2, pl.ds(1, 3), pl.ds(384, 1152), False)
    with jax.named_scope("slab"):
        for side, (row, is_pole) in enumerate(((0, lat == 0), (5, lat == 7))):
            received(hal.at[side], R_SLAB + side)

            @pl.when(jnp.logical_not(is_pole))
            def _():
                u[row, :, 0:90, :] = hal[side]

            @pl.when(is_pole)
            def _():
                u[row] = jnp.zeros((4, 96, 512), BF16)

        low = jnp.where(lat == 0, 0.0, 1.0)
        high = jnp.where(lat == 7, 0.0, 1.0)
        left_a, right_a = (edge_in[k, 1].astype(F32) * low for k in (0, 1))
        left_b, right_b = (edge_in[k, 2].astype(F32) * high for k in (0, 1))
        for b in range(4):
            put_edges(0, b, left_a[12 + b : 13 + b], right_a[12 + b : 13 + b])
            put_edges(5, b, left_b[b : b + 1], right_b[b : b + 1])
    with jax.named_scope("halo1"):
        product(1, pl.ds(5, 1), pl.ds(1152, 384), True)
    with jax.named_scope("rz0"):
        reduce_z(0)
    with jax.named_scope("halo2"):
        product(2, pl.ds(0, 1), pl.ds(0, 384), True)
    with jax.named_scope("rf1"):
        reduce_far(1)
    with jax.named_scope("rf2"):
        reduce_far(2)
    with jax.named_scope("gz3_old"):
        gather_z3(0)
        gather_far(0, -1, 1)
    with jax.named_scope("rn1"):
        reduce_near(1)
    with jax.named_scope("rn2"):
        reduce_near(2)
    with jax.named_scope("rl0"):
        reduce_last(0)
    with jax.named_scope("perms"):
        make_perms(perm, core)
        prod[0, :, 96:104, :] = jnp.zeros((4, 8, 512), F32)
    with jax.named_scope("gz4_old"):
        gather_z4(0)
        gather_far(0, -2, 2)
    with jax.named_scope("rz1"):
        reduce_z(1)
    with jax.named_scope("rz2"):
        reduce_z(2)
    with jax.named_scope("gfar_old"):
        gather_far(0, -3, 3, 4)
        gather_last(0, 0, -1, 1)
    with jax.named_scope("rl1"):
        reduce_last(1)
    with jax.named_scope("rl2"):
        reduce_last(2)
    with jax.named_scope("glast_old"):
        gather_last(0, -2, 2, -3, 3, 4)
        gather_end(0)
    with jax.named_scope("finish"):
        finish(0)
        finish(1)
        finish(2)

    g_sum = grad[...]
    nb[0] = jnp.zeros((1, 128), F32) + jnp.sum(g_sum * g_sum)
    for d in range(1, 16):
        send(nb.at[0], nl.at[0, d], S_N, R_N, plane_peers[d - 1])
    nl[0, 0] = nb[0]
    with jax.named_scope("natural_old"):

        @pl.loop(0, 9)
        def _(tap):
            natural(perm, old_m, old_o, wn, core, tap)

    with jax.named_scope("n0"):
        received(nl.at[0, pl.ds(1, 15)], R_N)
    plane_sum = jnp.sum(nl[0], axis=0)
    nb[1] = plane_sum
    for d in range(1, 16):
        send(nb.at[1], nl.at[1, d], S_N + 1, R_N + 1, line_peers[d - 1])
    nl[1, 0] = plane_sum
    with jax.named_scope("left_old"):
        left(edge_in, S_EDGE)
        left(hal, S_SLAB)
        for g in range(3):
            left(g_l.at[g], S_PAIR + g)
            left(lh.at[g], S_AH + g)
            left(lu.at[g], S_AU + g)
            left(l2.at[g], S_Z + g)
            left(fl.at[g, pl.ds(1, 7)], S_F + g)
        gather_left(0)
    with jax.named_scope("input0"):
        input_part(0)
    with jax.named_scope("n1"):
        received(nl.at[1, pl.ds(1, 15)], R_N + 1)
    square_sum = jnp.max(jnp.sum(nl[1], axis=0), axis=(0, 1), keepdims=True)
    max_norm = math.sqrt(float(CIN * TAPS * COUT))
    clip = jnp.minimum(1.0, max_norm / (jnp.sqrt(square_sum) + norm_eps))
    scaled = g_sum * clip.reshape(1, 1, 1)
    old = master[...]
    loads[0].wait()
    loads[1].wait()
    new_one = beta_one * one[...] + (1.0 - beta_one) * scaled
    new_two = beta_two * two[...] + (1.0 - beta_two) * scaled * scaled
    first_hat = new_one / (1.0 - beta_one**step_count)
    second_hat = new_two / (1.0 - beta_two**step_count)
    new_master = old - learn_rate * (
        first_hat / (jnp.sqrt(second_hat) + adam_eps) + decay_rate * old
    )
    wf[0] = new_master[:, :, 0:256]
    wf[1] = new_master[:, :, 256:512]
    gather_start(1)
    out_master[...] = new_master
    out_one[...] = new_one
    out_two[...] = new_two
    out_grad[...] = scaled
    with jax.named_scope("input1"):
        input_part(1)
    with jax.named_scope("gz"):
        gather_z(1)
    with jax.named_scope("input2"):
        input_part(2)
    with jax.named_scope("gz1"):
        gather_z1(1)
    with jax.named_scope("gz2"):
        gather_z2(1)
        gather_far(1, 0)
    with jax.named_scope("input3"):
        input_part(3)
    with jax.named_scope("gz3"):
        gather_z3(1)
    with jax.named_scope("gfar1"):
        gather_far(1, -1, 1)
        gather_last(1, 0)
    with jax.named_scope("gz4"):
        gather_z4(1)
    with jax.named_scope("gfar2"):
        gather_far(1, -2, 2)
        gather_last(1, -1, 1)
    with jax.named_scope("gfar3"):
        gather_far(1, -3, 3, 4)
    with jax.named_scope("glast"):
        gather_last(1, -2, 2, -3, 3, 4)
    with jax.named_scope("gend"):
        gather_end(1)
    with jax.named_scope("ends"):
        left(nl.at[0, pl.ds(1, 15)], S_N)
        left(nl.at[1, pl.ds(1, 15)], S_N + 1)
        gather_left(1)


def per_device(activations, upstream, master, moment_one, moment_two):
    fields = [
        pltpu.with_memory_space_constraint(jnp.transpose(v, (1, 0, 2, 3)), pltpu.VMEM)
        for v in (activations, upstream)
    ]
    state = [jnp.transpose(v, (1, 0, 2)) for v in (master, moment_one, moment_two)]
    vmem = pl.BlockSpec(memory_space=pltpu.VMEM)
    far = pl.BlockSpec(memory_space=pl.ANY)
    shard = jax.ShapeDtypeStruct((9, 2, 512), F32)
    block = pltpu.VMEM((4, 8, 9, 16, 256), BF16)
    held = pltpu.VMEM((9, 2, 512), F32)
    input_grad, *rest = pl.pallas_call(
        kernel,
        out_shape=(
            pltpu.VMEM((4, 4, 90, 512), BF16), block, block,
            held, held, held, held,
        ),
        in_specs=[vmem, vmem, vmem, far, far],
        out_specs=(vmem,) * 7,
        scratch_shapes=[
            pltpu.VMEM((9, 2, 512), F32),
            pltpu.VMEM((9, 2, 512), F32),
            pltpu.VMEM((6, 4, 96, 512), BF16),
            pltpu.VMEM((4, 4, 96, 512), BF16),
            pltpu.VMEM((3, 512, 1536), BF16),
            pltpu.VMEM((3, 512, 1536), BF16),
            pltpu.VMEM((2, 256, 256), BF16),
            pltpu.VMEM((2, 16, 512), F32),
            pltpu.VMEM((2, 16, 512), BF16),
            pltpu.VMEM((2, 3, 16, 512), BF16),
            pltpu.VMEM((2, 4, 90, 512), BF16),
            pltpu.VMEM((3, 3, 512, 256), F32),
            pltpu.VMEM((3, 3, 512, 256), F32),
            pltpu.VMEM((3, 3, 512, 256), F32),
            pltpu.VMEM((3, 2, 3, 64, 256), BF16),
            pltpu.VMEM((3, 2, 3, 64, 256), BF16),
            pltpu.VMEM((3, 2, 3, 128, 256), BF16),
            pltpu.VMEM((3, 2, 3, 128, 256), BF16),
            pltpu.VMEM((3, 8, 3, 16, 256), F32),
            pltpu.VMEM((3, 8, 3, 16, 256), BF16),
            pltpu.VMEM((3, 7, 3, 16, 256), BF16),
            pltpu.VMEM((3, 2, 4, 3, 2, 256), F32),
            pltpu.VMEM((3, 8, 3, 2, 256), F32),
            pltpu.VMEM((9, 2, 512), F32),
            pltpu.VMEM((2, 1, 128), F32),
            pltpu.VMEM((2, 16, 1, 128), F32),
            pltpu.VMEM((2, 9, 2, 256), F32),
            pltpu.VMEM((2, 8, 9, 2, 256), F32),
            pltpu.VMEM((9, 16, 256), F32),
            pltpu.VMEM((4, 8, 9, 16, 256), BF16),
            pltpu.VMEM((4, 8, 9, 16, 256), BF16),
            pltpu.VMEM((9, 512, 512), BF16),
            pltpu.VMEM((3, 4, 104, 512), F32),
            pltpu.SemaphoreType.DMA((2,)),
            pltpu.SemaphoreType.DMA((S_SLOTS,)),
            pltpu.SemaphoreType.DMA((R_SLOTS,)),
        ],
        compiler_params=pltpu.CompilerParams(
            collective_id=0, has_side_effects=True, vmem_limit_bytes=53 * 1024 * 1024
        ),
        name="conv_step",
    )(*fields, *state)
    outs = pl.pallas_call(
        finish_kernel,
        out_shape=(jax.ShapeDtypeStruct((9, 512, 512), BF16), shard, shard, shard, shard),
        in_specs=[vmem] * 6,
        out_specs=(far,) * 5,
        scratch_shapes=[
            pltpu.VMEM((9, 512, 512), BF16),
            pltpu.VMEM((2, 256, 256), BF16),
            pltpu.SemaphoreType.DMA((13,)),
        ],
        compiler_params=pltpu.CompilerParams(vmem_limit_bytes=8 * 1024 * 1024),
        name="finish_step",
    )(*rest)
    outs = [jnp.transpose(v, (1, 0, 2)) for v in outs]
    return (jnp.transpose(input_grad, (1, 0, 2, 3)), *outs)


def solution(mesh):
    field = P(None, "lat", "lon", None)
    state = P(("lat", "lon"), None, None)
    return jax.shard_map(
        per_device,
        mesh=mesh,
        in_specs=(field, field, state, state, state),
        out_specs=(field, P(), state, state, state, state),
        check_vma=False,
    )
```

```python
import functools
import math

import jax
import jax.numpy as jnp
from jax import lax
from jax.experimental import pallas as pl
from jax.experimental.pallas import tpu as pltpu
from jax.sharding import PartitionSpec as P

CIN = 512
COUT = 512
TAPS = 9

learn_rate = 0.01
beta_one = 0.9
beta_two = 0.999
adam_eps = 1e-08
decay_rate = 0.1
step_count = 10.0
norm_eps = 1e-06

F32 = jnp.float32
BF16 = jnp.bfloat16
MESH = pl.DeviceIdType.MESH

R_EDGE, R_SLAB, R_PAIR, R_A, R_Z, R_F, R_N = 0, 1, 3, 6, 18, 21, 24
R_LAST, R_GZ, R_NEAR, R_FAR, R_GP, R_EACH = 26, 27, 35, 51, 67, 42
S_EDGE, S_SLAB, S_PAIR, S_AH, S_AU, S_Z, S_F, S_N = 0, 1, 2, 5, 8, 11, 14, 17
S_LAST, S_GZ, S_NEAR, S_FAR, S_GP, S_EACH = 19, 20, 21, 22, 23, 5

ROW_ORDER = (1, 0, 2)


def nt_dot(a, b):
    return lax.dot_general(a, b, (((1,), (1,)), ((), ())), preferred_element_type=F32)


def nn_dot(a, b):
    return lax.dot_general(a, b, (((1,), (0,)), ((), ())), preferred_element_type=F32)


def ordered(channel, color):
    r = channel & 1
    core = (channel >> 1) & 1
    x = ((channel >> 2) & 1) * 2 + ((channel >> 8) & 1)
    z = (channel >> 3) & 7
    y = (channel >> 6) & 3
    first = y * (1 - color) + x * color
    last = x * (1 - color) + y * color
    return first * 128 + z * 16 + core * 8 + last * 2 + r


def block_order(place, color):
    r = place & 1
    last = (place >> 1) & 3
    core = (place >> 3) & 1
    z = (place >> 4) & 7
    high = place >> 7
    y_way = (last & 1) * 128 + high * 64 + z * 8 + (last >> 1) * 4 + core * 2 + r
    x_way = last * 64 + z * 8 + high * 4 + core * 2 + r
    return y_way * (1 - color) + x_way * color


def one_hot(mask):
    return jnp.where(mask, 1.0, 0.0).astype(BF16)


def make_perms(perm, core):
    rows = lax.broadcasted_iota(jnp.int32, (256, 256), 0)
    cols = lax.broadcasted_iota(jnp.int32, (1, 256), 1)
    perm[0] = one_hot(rows == block_order(cols, core))
    perm[1] = one_hot(rows == block_order(cols, 1 - core))


def natural(perm, w_m, w_o, dst, core, tap):
    for k, (w, color) in enumerate(((w_m, core), (w_o, 1 - core))):
        lanes = pl.ds(pl.multiple_of(color * 256, 256), 256)
        for parity in (0, 1):
            low = w[parity, :, tap].reshape(128, 256)
            high = w[parity + 2, :, tap].reshape(128, 256)
            got = jnp.concatenate([low, high], axis=0)
            block = nn_dot(perm[k], got).astype(BF16)
            for q in range(4):
                y_way = (q // 2) * 256 + (q % 2) * 128 + parity * 64
                x_way = parity * 256 + q * 64
                start = pl.multiple_of(y_way * (1 - color) + x_way * color, 64)
                dst[tap, pl.ds(start, 64), lanes] = block[q * 64 : (q + 1) * 64]


def finish_kernel(
    w_m, w_o, v0, v1, v2, v3, out_w, o0, o1, o2, o3, wn, perm, local
):
    core = lax.axis_index("lon") % 2
    copies = [
        pltpu.make_async_copy(v, o, local.at[k])
        for k, (v, o) in enumerate(((v0, o0), (v1, o1), (v2, o2), (v3, o3)))
    ]
    for copy in copies:
        copy.start()
    make_perms(perm, core)

    @pl.loop(0, 9)
    def _(tap):
        natural(perm, w_m, w_o, wn, core, tap)
        pltpu.make_async_copy(wn.at[tap], out_w.at[tap], local.at[4 + tap]).start()

    for copy in copies:
        copy.wait()
    for tap in range(9):
        pltpu.make_async_copy(wn.at[tap], out_w.at[tap], local.at[4 + tap]).wait()


def kernel(
    act, up, master, one_far, two_far,
    oi, new_m, new_o, out_master, out_one, out_two, out_grad,
    one, two, u, ap, at_m, at_o, perm, edge_f, edge, edge_in, hal,
    g_m, g_o, g_s, g_l, bh, lh, bu, lu, t1, b2, l2, fo, fl, grad, nb, nl,
    wf, wl, wt, old_m, old_o, wn, prod, local, ss, rs,
):
    lat = lax.axis_index("lat")
    lon = lax.axis_index("lon")
    x_lo, y = lat // 4, lat % 4
    z, x_hi, core = lon // 4, (lon // 2) % 2, lon % 2
    x = x_hi * 2 + x_lo

    def device(x_, y_, z_, core_):
        return ((x_ % 2) * 4 + y_, z_ * 4 + (x_ // 2) * 2 + core_)

    def along(color, step, core_):
        return device((x + step * color) % 4, (y + step * (1 - color)) % 4, z, core_)

    def z_peer(d):
        return device(x, y, (z + d) % 8, core)

    other = 1 - core
    sibling = device(x, y, z, other)
    after, before = along(core, 1, core), along(core, 3, core)
    first_me = y * (1 - core) + x * core
    last_me = x * (1 - core) + y * core

    def remote(src, dst, out_slot, in_slot, where):
        return pltpu.make_async_remote_copy(
            src_ref=src, dst_ref=dst, send_sem=ss.at[out_slot], recv_sem=rs.at[in_slot],
            device_id=where, device_id_type=MESH,
        )

    def send(src, dst, out_slot, in_slot, where):
        remote(src, dst, out_slot, in_slot, where).start()

    def received(dst, slot):
        remote(dst, dst, 0, slot, sibling).wait_recv()

    def left(src, slot):
        remote(src, src, slot, 0, sibling).wait_send()

    lanes_m = pl.ds(pl.multiple_of(core * 256, 256), 256)
    lanes_o = pl.ds(pl.multiple_of(other * 256, 256), 256)

    lat_down, lat_up = (lat + 1) % 8, (lat + 7) % 8
    lon_right, lon_left = (lon + 1) % 32, (lon + 31) % 32
    halo_peers = [
        (lat_down, lon), (lat_up, lon),
        (lat, lon_right), (lat_down, lon_right), (lat_up, lon_right),
        (lat, lon_left), (lat_down, lon_left), (lat_up, lon_left),
    ]
    plane_peers = [device((x + d // 4) % 4, (y + d % 4) % 4, z, core) for d in range(1, 16)]
    line_peers = [device(x, y, (z + d // 2) % 8, (core + d % 2) % 2) for d in range(1, 16)]
    cross_peers = [along(color, step, other) for color in (0, 1) for step in (1, 2, 3)]
    peers = halo_peers + plane_peers + line_peers + cross_peers
    barrier = pltpu.get_barrier_semaphore()
    for peer in peers:
        pl.semaphore_signal(barrier, inc=1, device_id=peer, device_id_type=MESH)

    loads = [
        pltpu.make_async_copy(src, dst, local.at[k])
        for k, (src, dst) in enumerate(
            ((one_far, one), (two_far, two))
        )
    ]
    for copy in loads:
        copy.start()
    wg_m, wg_o = (old_m, new_m), (old_o, new_o)
    wf[0] = master[:, :, 0:256]
    wf[1] = master[:, :, 256:512]
    for i in range(4):
        for b in range(4):
            g = i * 4 + b
            edge_f[0, g : g + 1, :] = up[i, b, 0:16, :].astype(F32)[0:1]
            edge_f[1, g : g + 1, :] = up[i, b, 80:90, :].astype(F32)[9:10]
    edge[...] = edge_f[...].astype(BF16)

    with jax.named_scope("barrier"):
        pl.semaphore_wait(barrier, len(peers))

    def gather_start(which):
        for dd in range(1, 8):
            da, dc = dd % 4, dd // 4
            color = core if dc == 0 else other
            here = x * (1 - color) + y * color
            send(
                wf.at[color], wl.at[which, core * 4 + here], which * S_EACH + S_LAST, which * R_EACH + R_LAST,
                along(1 - color, da, color),
            )
        wl[which, core * 4 + last_me] = wf[core]

    def piece(which, e, step=0):
        return wg_m[which].at[(first_me + 4 + step) % 4, (z + 8 + e) % 8]

    low_half, high_half = pl.ds(0, 128), pl.ds(128, 128)

    def to_pair(which, e, step):
        there = wg_o[which].at[(first_me + 4 + step) % 4, (z + 8 + e) % 8]
        send(piece(which, e, step), there, which * S_EACH + S_GP, which * R_EACH + R_GP, sibling)

    def gather_near(which, e, now=None):
        if not (which if now is None else now):
            return
        block = piece(which, e)
        send(block, block, which * S_EACH + S_NEAR, which * R_EACH + R_NEAR + 2 * (e % 8), after)
        send(block, block, which * S_EACH + S_NEAR, which * R_EACH + R_NEAR + 2 * (e % 8) + 1, before)
        to_pair(which, e, 0)

    def gather_z(which):
        received(wl.at[which, pl.ds(0, 7)], which * R_EACH + R_LAST)
        for k in range(8):
            wt[:, k * 2 : k * 2 + 2, :] = wl[which, k]
        wg_m[which][first_me, z] = wt[...].astype(BF16)
        mine = piece(which, 0)
        for k, d in enumerate((1, 7, 2, 6)):
            send(mine, mine, which * S_EACH + S_GZ, which * R_EACH + R_GZ + k, z_peer(d))
        gather_near(which, 0)

    def gather_z1(which):
        for k, e in enumerate((-1, 1)):
            received(piece(which, e), which * R_EACH + R_GZ + k)
            gather_near(which, e)

    def gather_z2(which):
        for k, e in enumerate((-2, 2)):
            block = piece(which, e)
            received(block, which * R_EACH + R_GZ + 2 + k)
            send(block, block, which * S_EACH + S_GZ, which * R_EACH + R_GZ + 4 + k, z_peer(1 if e < 0 else 7))
            gather_near(which, e)

    def gather_z3(which):
        for k, (e, half) in enumerate(((-3, low_half), (3, high_half))):
            block = piece(which, e)
            received(block, which * R_EACH + R_GZ + 4 + k)
            part = block.at[:, :, half]
            send(part, part, which * S_EACH + S_GZ, which * R_EACH + R_GZ + 6 + k, z_peer(1 if e < 0 else 7))
            gather_near(which, e)

    def gather_z4(which):
        block = piece(which, 4)
        received(block.at[:, :, low_half], which * R_EACH + R_GZ + 6)
        received(block.at[:, :, high_half], which * R_EACH + R_GZ + 7)
        gather_near(which, 4)

    def gather_far(which, *places):
        for e in places:
            for k, (step, half, where) in enumerate(
                ((-1, low_half, after), (1, high_half, before))
            ):
                block = piece(which, e, step)
                received(block, which * R_EACH + R_NEAR + 2 * (e % 8) + k)
                part = block.at[:, :, half]
                send(part, part, which * S_EACH + S_FAR, which * R_EACH + R_FAR + 2 * (e % 8) + k, where)
                to_pair(which, e, step)

    def gather_last(which, *places):
        for e in places:
            block = piece(which, e, 2)
            received(block.at[:, :, low_half], which * R_EACH + R_FAR + 2 * (e % 8))
            received(block.at[:, :, high_half], which * R_EACH + R_FAR + 2 * (e % 8) + 1)
            to_pair(which, e, 2)

    def gather_end(which):
        received(wg_o[which], which * R_EACH + R_GP)

    def gather_left(which):
        w = wg_m[which]
        left(w.at[0, pl.ds(0, 7)], which * S_EACH + S_GZ)
        left(w.at[pl.ds(0, 2)], which * S_EACH + S_NEAR)
        left(w.at[0], which * S_EACH + S_FAR)
        left(w, which * S_EACH + S_GP)

    gather_start(0)

    for k, where in enumerate(halo_peers[2:5]):
        send(edge.at[1], edge_in.at[0, k], S_EDGE, R_EDGE, where)
    for k, where in enumerate(halo_peers[5:8]):
        send(edge.at[0], edge_in.at[1, k], S_EDGE, R_EDGE, where)
    send(up.at[3], hal.at[0], S_SLAB, R_SLAB, halo_peers[0])
    send(up.at[0], hal.at[1], S_SLAB, R_SLAB + 1, halo_peers[1])

    ap[:, :, 80:96, :] = jnp.zeros((4, 4, 16, 512), BF16)
    ap[:, :, 0:90, :] = act[...]
    u[:, :, 80:96, :] = jnp.zeros((6, 4, 16, 512), BF16)
    u[1:5, :, 0:90, :] = up[...]
    rows = lax.broadcasted_iota(jnp.int32, (512, 512), 0)
    cols = lax.broadcasted_iota(jnp.int32, (1, 512), 1)
    group_end = lax.broadcasted_iota(jnp.int32, (512, 1536), 1) % 96 == 95
    act_all = ap[...].reshape(1536, 512)
    for color, at in ((other, at_o), (core, at_m)):
        pick = one_hot(rows == ordered(cols, color))
        base_at = nt_dot(pick, act_all)
        half_at = base_at.astype(BF16)
        at[1] = half_at
        at[0] = pltpu.roll(half_at, 1, 1)
        at[2] = jnp.where(group_end, pltpu.roll(half_at, 95, 1), pltpu.roll(half_at, 1535, 1))

    def put_edges(i, b, left, right):
        tile = u[i, b, 80:96, :].astype(F32)
        ids = lax.broadcasted_iota(jnp.int32, (16, 512), 0)
        tile = jnp.where(ids == 10, right, jnp.where(ids == 15, left, tile))
        u[i, b, 80:96, :] = tile.astype(BF16)

    with jax.named_scope("gz_old"):
        gather_z(0)
    with jax.named_scope("edges"):
        received(edge_in, R_EDGE)
        west, east = edge_in[0, 0].astype(F32), edge_in[1, 0].astype(F32)
        for i in range(4):
            for b in range(4):
                g = i * 4 + b
                put_edges(1 + i, b, west[g : g + 1], east[g : g + 1])

    def product(g, rows, cols, add):
        whole = add or g == 0

        @pl.loop(0, 3)
        def _(s):
            field = u[rows, :, :, lanes_o].reshape(-1, 256)
            term = nn_dot(at_o[s, :, cols], field)
            if add:
                term = term + g_o[g - 1, s]
            if whole:
                g_s[g, s] = term.astype(BF16)
            else:
                g_o[g - 1, s] = term

        if whole:
            send(g_s.at[g], g_l.at[g], S_PAIR + g, R_PAIR + g, sibling)

        @pl.loop(0, 3)
        def _(s):
            field = u[rows, :, :, lanes_m].reshape(-1, 256)
            term = nn_dot(at_m[s, :, cols], field)
            g_m[g, s] = g_m[g, s] + term if add else term

    def rows_of(step):
        return pl.ds(pl.multiple_of(((first_me + step) % 4) * 128, 128), 128)

    def reduce_far(g):
        received(g_l.at[g], R_PAIR + g)
        total = g_m[g, :, rows_of(2), :] + g_l[g, :, rows_of(2), :].astype(F32)
        bh[g, 0] = total[:, 0:64].astype(BF16)
        bh[g, 1] = total[:, 64:128].astype(BF16)
        send(bh.at[g, 0], lh.at[g, 0], S_AH + g, R_A + g * 4, after)
        send(bh.at[g, 1], lh.at[g, 1], S_AH + g, R_A + g * 4 + 1, before)

    def reduce_near(g):
        for k, (step, where) in enumerate(((1, after), (3, before))):
            total = g_m[g, :, rows_of(step), :] + g_l[g, :, rows_of(step), :].astype(F32)
            received(lh.at[g, k], R_A + g * 4 + k)
            came = lh[g, k].astype(F32)
            part = total[:, k * 64 : (k + 1) * 64] + came
            rest = total[:, (1 - k) * 64 : (2 - k) * 64]
            bu[g, k, :, k * 64 : (k + 1) * 64, :] = part.astype(BF16)
            bu[g, k, :, (1 - k) * 64 : (2 - k) * 64, :] = rest.astype(BF16)
            send(bu.at[g, k], lu.at[g, k], S_AU + g, R_A + g * 4 + 2 + k, where)

    def reduce_z(g):
        total = g_m[g, :, rows_of(0), :] + g_l[g, :, rows_of(0), :].astype(F32)
        for k in range(2):
            received(lu.at[g, k], R_A + g * 4 + 2 + k)
            total = total + lu[g, k].astype(F32)
        for k in range(8):
            part = total[:, k * 16 : (k + 1) * 16, :]
            t1[g, k] = part
            b2[g, k] = part.astype(BF16)
        for d in (4, 3, 5, 2, 6, 1, 7):
            send(b2.at[g, (z + d) % 8], l2.at[g, d - 1], S_Z + g, R_Z + g, z_peer(d))

    def reduce_last(g):
        received(l2.at[g], R_Z + g)
        total = t1[g, z]
        for d in range(7):
            total = total + l2[g, d].astype(F32)
        for c in range(2):
            for a in range(4):
                row = c * 8 + a * 2
                fo[g, c, a] = total[:, row : row + 2, :]
        fl[g, 0] = fo[g, core, last_me]
        for dd in range(1, 8):
            da, dc = dd % 4, dd // 4
            core_to = core if dc == 0 else other
            send(
                fo.at[g, core_to, (last_me + da) % 4], fl.at[g, dd],
                S_F + g, R_F + g, along(other, da, core_to),
            )

    def finish(g):
        r = ROW_ORDER[g]
        received(fl.at[g, pl.ds(1, 7)], R_F + g)
        grad[3 * r : 3 * r + 3, :, lanes_m] = (fl[g, 0] + fl[g, 1]) + (fl[g, 2] + fl[g, 3])
        grad[3 * r : 3 * r + 3, :, lanes_o] = (fl[g, 4] + fl[g, 5]) + (fl[g, 6] + fl[g, 7])

    def input_part(i):
        for s in range(3):
            total = nt_dot(u[i + 2].reshape(384, 512), wn[s])
            total = total + nt_dot(u[i + 1].reshape(384, 512), wn[3 + s])
            total = total + nt_dot(u[i].reshape(384, 512), wn[6 + s])
            total = total.reshape(4, 96, 512)
            if s == 2:
                prod[2, :, 8:104, :] = total
                prod[2, :, 7:8, :] = total[:, 95:96, :]
            else:
                prod[s, :, 0:96, :] = total
        for b in range(4):
            whole = prod[0, b, 1:97, :] + prod[1, b, 0:96, :] + prod[2, b, 7:103, :]
            oi[i, b] = whole[0:90].astype(BF16)

    with jax.named_scope("terms0"):
        product(0, pl.ds(1, 4), pl.ds(0, 1536), False)
    with jax.named_scope("gz1_old"):
        gather_z1(0)
    with jax.named_scope("rf0"):
        reduce_far(0)
    with jax.named_scope("own1"):
        product(1, pl.ds(2, 3), pl.ds(0, 1152), False)
    with jax.named_scope("gz2_old"):
        gather_z2(0)
    with jax.named_scope("own2"):
        product(2, pl.ds(1, 3), pl.ds(384, 1152), False)
    with jax.named_scope("slab"):
        for side, (row, is_pole) in enumerate(((0, lat == 0), (5, lat == 7))):
            received(hal.at[side], R_SLAB + side)

            @pl.when(jnp.logical_not(is_pole))
            def _():
                u[row, :, 0:90, :] = hal[side]

            @pl.when(is_pole)
            def _():
                u[row] = jnp.zeros((4, 96, 512), BF16)

        low = jnp.where(lat == 0, 0.0, 1.0)
        high = jnp.where(lat == 7, 0.0, 1.0)
        left_a, right_a = (edge_in[k, 1].astype(F32) * low for k in (0, 1))
        left_b, right_b = (edge_in[k, 2].astype(F32) * high for k in (0, 1))
        for b in range(4):
            put_edges(0, b, left_a[12 + b : 13 + b], right_a[12 + b : 13 + b])
            put_edges(5, b, left_b[b : b + 1], right_b[b : b + 1])
    with jax.named_scope("halo1"):
        product(1, pl.ds(5, 1), pl.ds(1152, 384), True)
    with jax.named_scope("halo2"):
        product(2, pl.ds(0, 1), pl.ds(0, 384), True)
    with jax.named_scope("rn0"):
        reduce_near(0)
    with jax.named_scope("rf1"):
        reduce_far(1)
    with jax.named_scope("rf2"):
        reduce_far(2)
    with jax.named_scope("gz3_old"):
        gather_z3(0)
    with jax.named_scope("perms"):
        make_perms(perm, core)
        prod[0, :, 96:104, :] = jnp.zeros((4, 8, 512), F32)
    with jax.named_scope("rn1"):
        reduce_near(1)
    with jax.named_scope("rn2"):
        reduce_near(2)
    with jax.named_scope("rz0"):
        reduce_z(0)
    with jax.named_scope("near_old"):
        gather_near(0, 0, True)
        gather_near(0, -1, True)
        gather_near(0, 1, True)
        gather_near(0, -2, True)
        gather_near(0, 2, True)
        gather_near(0, -3, True)
        gather_near(0, 3, True)
    with jax.named_scope("rz1"):
        reduce_z(1)
    with jax.named_scope("rz2"):
        reduce_z(2)
    with jax.named_scope("rl0"):
        reduce_last(0)
    with jax.named_scope("z4_old"):
        gather_z4(0)
        gather_near(0, 4, True)
    with jax.named_scope("rl1"):
        reduce_last(1)
    with jax.named_scope("rl2"):
        reduce_last(2)
    with jax.named_scope("finish"):
        finish(0)
        finish(1)
        finish(2)

    g_sum = grad[...]
    nb[0] = jnp.zeros((1, 128), F32) + jnp.sum(g_sum * g_sum)
    for d in range(1, 16):
        send(nb.at[0], nl.at[0, d], S_N, R_N, plane_peers[d - 1])
    nl[0, 0] = nb[0]
    with jax.named_scope("gfar_old"):
        gather_far(0, 0, -1, 1, -2, 2, -3, 3, 4)
    with jax.named_scope("n0"):
        received(nl.at[0, pl.ds(1, 15)], R_N)
    plane_sum = jnp.sum(nl[0], axis=0)
    nb[1] = plane_sum
    for d in range(1, 16):
        send(nb.at[1], nl.at[1, d], S_N + 1, R_N + 1, line_peers[d - 1])
    nl[1, 0] = plane_sum
    with jax.named_scope("glast_old"):
        gather_last(0, 0, -1, 1, -2, 2, -3, 3, 4)
    with jax.named_scope("n1"):
        received(nl.at[1, pl.ds(1, 15)], R_N + 1)
    square_sum = jnp.max(jnp.sum(nl[1], axis=0), axis=(0, 1), keepdims=True)
    max_norm = math.sqrt(float(CIN * TAPS * COUT))
    clip = jnp.minimum(1.0, max_norm / (jnp.sqrt(square_sum) + norm_eps))
    scaled = g_sum * clip.reshape(1, 1, 1)
    old = master[...]
    loads[0].wait()
    loads[1].wait()
    new_one = beta_one * one[...] + (1.0 - beta_one) * scaled
    new_two = beta_two * two[...] + (1.0 - beta_two) * scaled * scaled
    first_hat = new_one / (1.0 - beta_one**step_count)
    second_hat = new_two / (1.0 - beta_two**step_count)
    new_master = old - learn_rate * (
        first_hat / (jnp.sqrt(second_hat) + adam_eps) + decay_rate * old
    )
    left(wl.at[0, pl.ds(0, 7)], S_LAST)
    wf[0] = new_master[:, :, 0:256]
    wf[1] = new_master[:, :, 256:512]
    gather_start(1)
    out_master[...] = new_master
    out_one[...] = new_one
    out_two[...] = new_two
    out_grad[...] = scaled
    with jax.named_scope("gend_old"):
        gather_end(0)
    with jax.named_scope("natural_old"):

        @pl.loop(0, 9)
        def _(tap):
            natural(perm, old_m, old_o, wn, core, tap)

    with jax.named_scope("gz"):
        gather_z(1)
    with jax.named_scope("input0"):
        input_part(0)
    with jax.named_scope("input1"):
        input_part(1)
    with jax.named_scope("gz1"):
        gather_z1(1)
    with jax.named_scope("input2"):
        input_part(2)
    with jax.named_scope("gz2"):
        gather_z2(1)
        gather_far(1, 0)
    with jax.named_scope("gz3"):
        gather_z3(1)
    with jax.named_scope("gfar1"):
        gather_far(1, -1, 1)
        gather_last(1, 0)
    with jax.named_scope("gz4"):
        gather_z4(1)
    with jax.named_scope("input3"):
        input_part(3)
    with jax.named_scope("gfar2"):
        gather_far(1, -2, 2)
        gather_last(1, -1, 1)
    with jax.named_scope("gfar3"):
        gather_far(1, -3, 3, 4)
    with jax.named_scope("glast"):
        gather_last(1, -2, 2, -3, 3, 4)
    with jax.named_scope("gend"):
        gather_end(1)
    with jax.named_scope("ends"):
        left(edge_in, S_EDGE)
        left(hal, S_SLAB)
        for g in range(3):
            left(g_l.at[g], S_PAIR + g)
            left(lh.at[g], S_AH + g)
            left(lu.at[g], S_AU + g)
            left(l2.at[g], S_Z + g)
            left(fl.at[g, pl.ds(1, 7)], S_F + g)
        for k in range(2):
            left(nl.at[k, pl.ds(1, 15)], S_N + k)
        gather_left(0)
        gather_left(1)
        left(wl.at[1, pl.ds(0, 7)], S_EACH + S_LAST)


def per_device(activations, upstream, master, moment_one, moment_two):
    fields = [
        pltpu.with_memory_space_constraint(jnp.transpose(v, (1, 0, 2, 3)), pltpu.VMEM)
        for v in (activations, upstream)
    ]
    state = [jnp.transpose(v, (1, 0, 2)) for v in (master, moment_one, moment_two)]
    vmem = pl.BlockSpec(memory_space=pltpu.VMEM)
    far = pl.BlockSpec(memory_space=pl.ANY)
    shard = jax.ShapeDtypeStruct((9, 2, 512), F32)
    block = pltpu.VMEM((4, 8, 9, 16, 256), BF16)
    held = pltpu.VMEM((9, 2, 512), F32)
    input_grad, *rest = pl.pallas_call(
        kernel,
        out_shape=(
            pltpu.VMEM((4, 4, 90, 512), BF16), block, block,
            held, held, held, held,
        ),
        in_specs=[vmem, vmem, vmem, far, far],
        out_specs=(vmem,) * 7,
        scratch_shapes=[
            pltpu.VMEM((9, 2, 512), F32),
            pltpu.VMEM((9, 2, 512), F32),
            pltpu.VMEM((6, 4, 96, 512), BF16),
            pltpu.VMEM((4, 4, 96, 512), BF16),
            pltpu.VMEM((3, 512, 1536), BF16),
            pltpu.VMEM((3, 512, 1536), BF16),
            pltpu.VMEM((2, 256, 256), BF16),
            pltpu.VMEM((2, 16, 512), F32),
            pltpu.VMEM((2, 16, 512), BF16),
            pltpu.VMEM((2, 3, 16, 512), BF16),
            pltpu.VMEM((2, 4, 90, 512), BF16),
            pltpu.VMEM((3, 3, 512, 256), F32),
            pltpu.VMEM((2, 3, 512, 256), F32),
            pltpu.VMEM((3, 3, 512, 256), BF16),
            pltpu.VMEM((3, 3, 512, 256), BF16),
            pltpu.VMEM((3, 2, 3, 64, 256), BF16),
            pltpu.VMEM((3, 2, 3, 64, 256), BF16),
            pltpu.VMEM((3, 2, 3, 128, 256), BF16),
            pltpu.VMEM((3, 2, 3, 128, 256), BF16),
            pltpu.VMEM((3, 8, 3, 16, 256), F32),
            pltpu.VMEM((3, 8, 3, 16, 256), BF16),
            pltpu.VMEM((3, 7, 3, 16, 256), BF16),
            pltpu.VMEM((3, 2, 4, 3, 2, 256), F32),
            pltpu.VMEM((3, 8, 3, 2, 256), F32),
            pltpu.VMEM((9, 2, 512), F32),
            pltpu.VMEM((2, 1, 128), F32),
            pltpu.VMEM((2, 16, 1, 128), F32),
            pltpu.VMEM((2, 9, 2, 256), F32),
            pltpu.VMEM((2, 8, 9, 2, 256), F32),
            pltpu.VMEM((9, 16, 256), F32),
            pltpu.VMEM((4, 8, 9, 16, 256), BF16),
            pltpu.VMEM((4, 8, 9, 16, 256), BF16),
            pltpu.VMEM((9, 512, 512), BF16),
            pltpu.VMEM((3, 4, 104, 512), F32),
            pltpu.SemaphoreType.DMA((2,)),
            pltpu.SemaphoreType.DMA((S_LAST + 2 * S_EACH,)),
            pltpu.SemaphoreType.DMA((R_LAST + 2 * R_EACH,)),
        ],
        compiler_params=pltpu.CompilerParams(
            collective_id=0, has_side_effects=True, vmem_limit_bytes=53 * 1024 * 1024
        ),
        name="conv_step",
    )(*fields, *state)
    outs = pl.pallas_call(
        finish_kernel,
        out_shape=(jax.ShapeDtypeStruct((9, 512, 512), BF16), shard, shard, shard, shard),
        in_specs=[vmem] * 6,
        out_specs=(far,) * 5,
        scratch_shapes=[
            pltpu.VMEM((9, 512, 512), BF16),
            pltpu.VMEM((2, 256, 256), BF16),
            pltpu.SemaphoreType.DMA((13,)),
        ],
        compiler_params=pltpu.CompilerParams(vmem_limit_bytes=8 * 1024 * 1024),
        name="finish_step",
    )(*rest)
    outs = [jnp.transpose(v, (1, 0, 2)) for v in outs]
    return (jnp.transpose(input_grad, (1, 0, 2, 3)), *outs)


def solution(mesh):
    field = P(None, "lat", "lon", None)
    state = P(("lat", "lon"), None, None)
    return jax.shard_map(
        per_device,
        mesh=mesh,
        in_specs=(field, field, state, state, state),
        out_specs=(field, P(), state, state, state, state),
        check_vma=False,
    )
```

```python
import functools
import math

import jax
import jax.numpy as jnp
from jax import lax
from jax.experimental import pallas as pl
from jax.experimental.pallas import tpu as pltpu
from jax.sharding import PartitionSpec as P

CIN = 512
COUT = 512
TAPS = 9

learn_rate = 0.01
beta_one = 0.9
beta_two = 0.999
adam_eps = 1e-08
decay_rate = 0.1
step_count = 10.0
norm_eps = 1e-06

F32 = jnp.float32
BF16 = jnp.bfloat16
MESH = pl.DeviceIdType.MESH

R_EDGE, R_SLAB, R_PAIR, R_A, R_Z, R_F, R_N = 0, 1, 3, 6, 18, 21, 24
R_LAST, R_GZ, R_NEAR, R_FAR, R_GP, R_EACH = 26, 27, 35, 51, 67, 42
S_EDGE, S_SLAB, S_PAIR, S_AH, S_AU, S_Z, S_F, S_N = 0, 1, 2, 5, 8, 11, 14, 17
S_LAST, S_GZ, S_NEAR, S_FAR, S_GP, S_EACH = 19, 20, 21, 22, 23, 5

ROW_ORDER = (1, 0, 2)


def nt_dot(a, b):
    return lax.dot_general(a, b, (((1,), (1,)), ((), ())), preferred_element_type=F32)


def nn_dot(a, b):
    return lax.dot_general(a, b, (((1,), (0,)), ((), ())), preferred_element_type=F32)


def ordered(channel, color):
    r = channel & 1
    core = (channel >> 1) & 1
    x = ((channel >> 2) & 1) * 2 + ((channel >> 8) & 1)
    z = (channel >> 3) & 7
    y = (channel >> 6) & 3
    first = y * (1 - color) + x * color
    last = x * (1 - color) + y * color
    return first * 128 + z * 16 + core * 8 + last * 2 + r


def block_order(place, color):
    r = place & 1
    last = (place >> 1) & 3
    core = (place >> 3) & 1
    z = (place >> 4) & 7
    high = place >> 7
    y_way = (last & 1) * 128 + high * 64 + z * 8 + (last >> 1) * 4 + core * 2 + r
    x_way = last * 64 + z * 8 + high * 4 + core * 2 + r
    return y_way * (1 - color) + x_way * color


def one_hot(mask):
    return jnp.where(mask, 1.0, 0.0).astype(BF16)


def make_perms(perm, core):
    rows = lax.broadcasted_iota(jnp.int32, (256, 256), 0)
    cols = lax.broadcasted_iota(jnp.int32, (1, 256), 1)
    perm[0] = one_hot(rows == block_order(cols, core))
    perm[1] = one_hot(rows == block_order(cols, 1 - core))


def natural(perm, w_m, w_o, dst, core, tap):
    for k, (w, color) in enumerate(((w_m, core), (w_o, 1 - core))):
        lanes = pl.ds(pl.multiple_of(color * 256, 256), 256)
        for parity in (0, 1):
            low = w[parity, :, tap].reshape(128, 256)
            high = w[parity + 2, :, tap].reshape(128, 256)
            got = jnp.concatenate([low, high], axis=0)
            block = nn_dot(perm[k], got).astype(BF16)
            for q in range(4):
                y_way = (q // 2) * 256 + (q % 2) * 128 + parity * 64
                x_way = parity * 256 + q * 64
                start = pl.multiple_of(y_way * (1 - color) + x_way * color, 64)
                dst[tap, pl.ds(start, 64), lanes] = block[q * 64 : (q + 1) * 64]


def finish_kernel(
    w_m, w_o, v0, v1, v2, v3, out_w, o0, o1, o2, o3, wn, perm, local
):
    core = lax.axis_index("lon") % 2
    copies = [
        pltpu.make_async_copy(v, o, local.at[k])
        for k, (v, o) in enumerate(((v0, o0), (v1, o1), (v2, o2), (v3, o3)))
    ]
    for copy in copies:
        copy.start()
    make_perms(perm, core)

    @pl.loop(0, 9)
    def _(tap):
        natural(perm, w_m, w_o, wn, core, tap)
        pltpu.make_async_copy(wn.at[tap], out_w.at[tap], local.at[4 + tap]).start()

    for copy in copies:
        copy.wait()
    for tap in range(9):
        pltpu.make_async_copy(wn.at[tap], out_w.at[tap], local.at[4 + tap]).wait()


def kernel(
    act, up, master, one_far, two_far,
    oi, new_m, new_o, out_master, out_one, out_two, out_grad,
    one, two, u, ap, at_m, at_o, perm, edge_f, edge, edge_in, hal,
    g_m, g_o, g_s, g_l, bh, lh, bu, lu, t1, b2, l2, fo, fl, grad, nb, nl,
    wf, wl, wt, old_m, old_o, wn, prod, local, ss, rs,
):
    lat = lax.axis_index("lat")
    lon = lax.axis_index("lon")
    x_lo, y = lat // 4, lat % 4
    z, x_hi, core = lon // 4, (lon // 2) % 2, lon % 2
    x = x_hi * 2 + x_lo

    def device(x_, y_, z_, core_):
        return ((x_ % 2) * 4 + y_, z_ * 4 + (x_ // 2) * 2 + core_)

    def along(color, step, core_):
        return device((x + step * color) % 4, (y + step * (1 - color)) % 4, z, core_)

    def z_peer(d):
        return device(x, y, (z + d) % 8, core)

    other = 1 - core
    sibling = device(x, y, z, other)
    after, before = along(core, 1, core), along(core, 3, core)
    first_me = y * (1 - core) + x * core
    last_me = x * (1 - core) + y * core

    def remote(src, dst, out_slot, in_slot, where):
        return pltpu.make_async_remote_copy(
            src_ref=src, dst_ref=dst, send_sem=ss.at[out_slot], recv_sem=rs.at[in_slot],
            device_id=where, device_id_type=MESH,
        )

    def send(src, dst, out_slot, in_slot, where):
        remote(src, dst, out_slot, in_slot, where).start()

    def received(dst, slot):
        remote(dst, dst, 0, slot, sibling).wait_recv()

    def left(src, slot):
        remote(src, src, slot, 0, sibling).wait_send()

    lanes_m = pl.ds(pl.multiple_of(core * 256, 256), 256)
    lanes_o = pl.ds(pl.multiple_of(other * 256, 256), 256)

    lat_down, lat_up = (lat + 1) % 8, (lat + 7) % 8
    lon_right, lon_left = (lon + 1) % 32, (lon + 31) % 32
    halo_peers = [
        (lat_down, lon), (lat_up, lon),
        (lat, lon_right), (lat_down, lon_right), (lat_up, lon_right),
        (lat, lon_left), (lat_down, lon_left), (lat_up, lon_left),
    ]
    plane_peers = [device((x + d // 4) % 4, (y + d % 4) % 4, z, core) for d in range(1, 16)]
    line_peers = [device(x, y, (z + d // 2) % 8, (core + d % 2) % 2) for d in range(1, 16)]
    cross_peers = [along(color, step, other) for color in (0, 1) for step in (1, 2, 3)]
    peers = halo_peers + plane_peers + line_peers + cross_peers
    barrier = pltpu.get_barrier_semaphore()
    for peer in peers:
        pl.semaphore_signal(barrier, inc=1, device_id=peer, device_id_type=MESH)

    loads = [
        pltpu.make_async_copy(src, dst, local.at[k])
        for k, (src, dst) in enumerate(
            ((one_far, one), (two_far, two))
        )
    ]
    for copy in loads:
        copy.start()
    wg_m, wg_o = (old_m, new_m), (old_o, new_o)
    wf[0] = master[:, :, 0:256]
    wf[1] = master[:, :, 256:512]
    for i in range(4):
        for b in range(4):
            g = i * 4 + b
            edge_f[0, g : g + 1, :] = up[i, b, 0:16, :].astype(F32)[0:1]
            edge_f[1, g : g + 1, :] = up[i, b, 80:90, :].astype(F32)[9:10]
    edge[...] = edge_f[...].astype(BF16)

    with jax.named_scope("barrier"):
        pl.semaphore_wait(barrier, len(peers))

    def gather_start(which):
        for dd in range(1, 8):
            da, dc = dd % 4, dd // 4
            color = core if dc == 0 else other
            here = x * (1 - color) + y * color
            send(
                wf.at[color], wl.at[which, core * 4 + here], which * S_EACH + S_LAST, which * R_EACH + R_LAST,
                along(1 - color, da, color),
            )
        wl[which, core * 4 + last_me] = wf[core]

    def piece(which, e, step=0):
        return wg_m[which].at[(first_me + 4 + step) % 4, (z + 8 + e) % 8]

    low_half, high_half = pl.ds(0, 128), pl.ds(128, 128)

    def to_pair(which, e, step):
        there = wg_o[which].at[(first_me + 4 + step) % 4, (z + 8 + e) % 8]
        send(piece(which, e, step), there, which * S_EACH + S_GP, which * R_EACH + R_GP, sibling)

    def gather_near(which, e, now=None):
        if not (which if now is None else now):
            return
        block = piece(which, e)
        send(block, block, which * S_EACH + S_NEAR, which * R_EACH + R_NEAR + 2 * (e % 8), after)
        send(block, block, which * S_EACH + S_NEAR, which * R_EACH + R_NEAR + 2 * (e % 8) + 1, before)
        to_pair(which, e, 0)

    def gather_z(which):
        received(wl.at[which, pl.ds(0, 7)], which * R_EACH + R_LAST)
        for k in range(8):
            wt[:, k * 2 : k * 2 + 2, :] = wl[which, k]
        wg_m[which][first_me, z] = wt[...].astype(BF16)
        mine = piece(which, 0)
        for k, d in enumerate((1, 7, 2, 6)):
            send(mine, mine, which * S_EACH + S_GZ, which * R_EACH + R_GZ + k, z_peer(d))
        gather_near(which, 0)

    def gather_z1(which):
        for k, e in enumerate((-1, 1)):
            received(piece(which, e), which * R_EACH + R_GZ + k)
            gather_near(which, e)

    def gather_z2(which):
        for k, e in enumerate((-2, 2)):
            block = piece(which, e)
            received(block, which * R_EACH + R_GZ + 2 + k)
            send(block, block, which * S_EACH + S_GZ, which * R_EACH + R_GZ + 4 + k, z_peer(1 if e < 0 else 7))
            gather_near(which, e)

    def gather_z3(which):
        for k, (e, half) in enumerate(((-3, low_half), (3, high_half))):
            block = piece(which, e)
            received(block, which * R_EACH + R_GZ + 4 + k)
            part = block.at[:, :, half]
            send(part, part, which * S_EACH + S_GZ, which * R_EACH + R_GZ + 6 + k, z_peer(1 if e < 0 else 7))
            gather_near(which, e)

    def gather_z4(which):
        block = piece(which, 4)
        received(block.at[:, :, low_half], which * R_EACH + R_GZ + 6)
        received(block.at[:, :, high_half], which * R_EACH + R_GZ + 7)
        gather_near(which, 4)

    def gather_far(which, *places):
        for e in places:
            for k, (step, half, where) in enumerate(
                ((-1, low_half, after), (1, high_half, before))
            ):
                block = piece(which, e, step)
                received(block, which * R_EACH + R_NEAR + 2 * (e % 8) + k)
                part = block.at[:, :, half]
                send(part, part, which * S_EACH + S_FAR, which * R_EACH + R_FAR + 2 * (e % 8) + k, where)
                to_pair(which, e, step)

    def gather_last(which, *places):
        for e in places:
            block = piece(which, e, 2)
            received(block.at[:, :, low_half], which * R_EACH + R_FAR + 2 * (e % 8))
            received(block.at[:, :, high_half], which * R_EACH + R_FAR + 2 * (e % 8) + 1)
            to_pair(which, e, 2)

    def gather_end(which):
        received(wg_o[which], which * R_EACH + R_GP)

    def gather_left(which):
        w = wg_m[which]
        left(w.at[0, pl.ds(0, 7)], which * S_EACH + S_GZ)
        left(w.at[pl.ds(0, 2)], which * S_EACH + S_NEAR)
        left(w.at[0], which * S_EACH + S_FAR)
        left(w, which * S_EACH + S_GP)

    gather_start(0)

    for k, where in enumerate(halo_peers[2:5]):
        send(edge.at[1], edge_in.at[0, k], S_EDGE, R_EDGE, where)
    for k, where in enumerate(halo_peers[5:8]):
        send(edge.at[0], edge_in.at[1, k], S_EDGE, R_EDGE, where)
    send(up.at[3], hal.at[0], S_SLAB, R_SLAB, halo_peers[0])
    send(up.at[0], hal.at[1], S_SLAB, R_SLAB + 1, halo_peers[1])

    ap[:, :, 80:96, :] = jnp.zeros((4, 4, 16, 512), BF16)
    ap[:, :, 0:90, :] = act[...]
    u[:, :, 80:96, :] = jnp.zeros((6, 4, 16, 512), BF16)
    u[1:5, :, 0:90, :] = up[...]
    rows = lax.broadcasted_iota(jnp.int32, (512, 512), 0)
    cols = lax.broadcasted_iota(jnp.int32, (1, 512), 1)
    group_end = lax.broadcasted_iota(jnp.int32, (512, 1536), 1) % 96 == 95
    act_all = ap[...].reshape(1536, 512)
    for color, at in ((other, at_o), (core, at_m)):
        pick = one_hot(rows == ordered(cols, color))
        base_at = nt_dot(pick, act_all)
        half_at = base_at.astype(BF16)
        at[1] = half_at
        at[0] = pltpu.roll(half_at, 1, 1)
        at[2] = jnp.where(group_end, pltpu.roll(half_at, 95, 1), pltpu.roll(half_at, 1535, 1))

    def put_edges(i, b, left, right):
        tile = u[i, b, 80:96, :].astype(F32)
        ids = lax.broadcasted_iota(jnp.int32, (16, 512), 0)
        tile = jnp.where(ids == 10, right, jnp.where(ids == 15, left, tile))
        u[i, b, 80:96, :] = tile.astype(BF16)

    with jax.named_scope("edges"):
        received(edge_in, R_EDGE)
        west, east = edge_in[0, 0].astype(F32), edge_in[1, 0].astype(F32)
        for i in range(4):
            for b in range(4):
                g = i * 4 + b
                put_edges(1 + i, b, west[g : g + 1], east[g : g + 1])

    def product(g, rows, cols, add):
        whole = add or g == 0

        @pl.loop(0, 3)
        def _(s):
            field = u[rows, :, :, lanes_o].reshape(-1, 256)
            term = nn_dot(at_o[s, :, cols], field)
            if add:
                term = term + g_o[g - 1, s]
            if whole:
                g_s[g, s] = term.astype(BF16)
            else:
                g_o[g - 1, s] = term

        if whole:
            send(g_s.at[g], g_l.at[g], S_PAIR + g, R_PAIR + g, sibling)

        @pl.loop(0, 3)
        def _(s):
            field = u[rows, :, :, lanes_m].reshape(-1, 256)
            term = nn_dot(at_m[s, :, cols], field)
            g_m[g, s] = g_m[g, s] + term if add else term

    def rows_of(step):
        return pl.ds(pl.multiple_of(((first_me + step) % 4) * 128, 128), 128)

    def reduce_far(g):
        received(g_l.at[g], R_PAIR + g)
        total = g_m[g, :, rows_of(2), :] + g_l[g, :, rows_of(2), :].astype(F32)
        bh[g, 0] = total[:, 0:64].astype(BF16)
        bh[g, 1] = total[:, 64:128].astype(BF16)
        send(bh.at[g, 0], lh.at[g, 0], S_AH + g, R_A + g * 4, after)
        send(bh.at[g, 1], lh.at[g, 1], S_AH + g, R_A + g * 4 + 1, before)

    def reduce_near(g):
        for k, (step, where) in enumerate(((1, after), (3, before))):
            total = g_m[g, :, rows_of(step), :] + g_l[g, :, rows_of(step), :].astype(F32)
            received(lh.at[g, k], R_A + g * 4 + k)
            came = lh[g, k].astype(F32)
            part = total[:, k * 64 : (k + 1) * 64] + came
            rest = total[:, (1 - k) * 64 : (2 - k) * 64]
            bu[g, k, :, k * 64 : (k + 1) * 64, :] = part.astype(BF16)
            bu[g, k, :, (1 - k) * 64 : (2 - k) * 64, :] = rest.astype(BF16)
            send(bu.at[g, k], lu.at[g, k], S_AU + g, R_A + g * 4 + 2 + k, where)

    def reduce_z(g):
        total = g_m[g, :, rows_of(0), :] + g_l[g, :, rows_of(0), :].astype(F32)
        for k in range(2):
            received(lu.at[g, k], R_A + g * 4 + 2 + k)
            total = total + lu[g, k].astype(F32)
        for k in range(8):
            part = total[:, k * 16 : (k + 1) * 16, :]
            t1[g, k] = part
            b2[g, k] = part.astype(BF16)
        for d in (4, 3, 5, 2, 6, 1, 7):
            send(b2.at[g, (z + d) % 8], l2.at[g, d - 1], S_Z + g, R_Z + g, z_peer(d))

    def reduce_last(g):
        received(l2.at[g], R_Z + g)
        total = t1[g, z]
        for d in range(7):
            total = total + l2[g, d].astype(F32)
        for c in range(2):
            for a in range(4):
                row = c * 8 + a * 2
                fo[g, c, a] = total[:, row : row + 2, :]
        fl[g, 0] = fo[g, core, last_me]
        for dd in range(1, 8):
            da, dc = dd % 4, dd // 4
            core_to = core if dc == 0 else other
            send(
                fo.at[g, core_to, (last_me + da) % 4], fl.at[g, dd],
                S_F + g, R_F + g, along(other, da, core_to),
            )

    def finish(g):
        r = ROW_ORDER[g]
        received(fl.at[g, pl.ds(1, 7)], R_F + g)
        grad[3 * r : 3 * r + 3, :, lanes_m] = (fl[g, 0] + fl[g, 1]) + (fl[g, 2] + fl[g, 3])
        grad[3 * r : 3 * r + 3, :, lanes_o] = (fl[g, 4] + fl[g, 5]) + (fl[g, 6] + fl[g, 7])

    def input_part(i):
        for s in range(3):
            total = nt_dot(u[i + 2].reshape(384, 512), wn[s])
            total = total + nt_dot(u[i + 1].reshape(384, 512), wn[3 + s])
            total = total + nt_dot(u[i].reshape(384, 512), wn[6 + s])
            total = total.reshape(4, 96, 512)
            if s == 2:
                prod[2, :, 8:104, :] = total
                prod[2, :, 7:8, :] = total[:, 95:96, :]
            else:
                prod[s, :, 0:96, :] = total
        for b in range(4):
            whole = prod[0, b, 1:97, :] + prod[1, b, 0:96, :] + prod[2, b, 7:103, :]
            oi[i, b] = whole[0:90].astype(BF16)

    with jax.named_scope("terms0"):
        product(0, pl.ds(1, 4), pl.ds(0, 1536), False)
    with jax.named_scope("own1"):
        product(1, pl.ds(2, 3), pl.ds(0, 1152), False)
    with jax.named_scope("rf0"):
        reduce_far(0)
    with jax.named_scope("own2"):
        product(2, pl.ds(1, 3), pl.ds(384, 1152), False)
    with jax.named_scope("gz_old"):
        gather_z(0)
    with jax.named_scope("slab"):
        for side, (row, is_pole) in enumerate(((0, lat == 0), (5, lat == 7))):
            received(hal.at[side], R_SLAB + side)

            @pl.when(jnp.logical_not(is_pole))
            def _():
                u[row, :, 0:90, :] = hal[side]

            @pl.when(is_pole)
            def _():
                u[row] = jnp.zeros((4, 96, 512), BF16)

        low = jnp.where(lat == 0, 0.0, 1.0)
        high = jnp.where(lat == 7, 0.0, 1.0)
        left_a, right_a = (edge_in[k, 1].astype(F32) * low for k in (0, 1))
        left_b, right_b = (edge_in[k, 2].astype(F32) * high for k in (0, 1))
        for b in range(4):
            put_edges(0, b, left_a[12 + b : 13 + b], right_a[12 + b : 13 + b])
            put_edges(5, b, left_b[b : b + 1], right_b[b : b + 1])
    with jax.named_scope("halo1"):
        product(1, pl.ds(5, 1), pl.ds(1152, 384), True)
    with jax.named_scope("halo2"):
        product(2, pl.ds(0, 1), pl.ds(0, 384), True)
    with jax.named_scope("rn0"):
        reduce_near(0)
    with jax.named_scope("rf1"):
        reduce_far(1)
    with jax.named_scope("rf2"):
        reduce_far(2)
    with jax.named_scope("perms"):
        make_perms(perm, core)
        prod[0, :, 96:104, :] = jnp.zeros((4, 8, 512), F32)
    with jax.named_scope("rn1"):
        reduce_near(1)
    with jax.named_scope("rn2"):
        reduce_near(2)
    with jax.named_scope("rz0"):
        reduce_z(0)
    with jax.named_scope("gz1_old"):
        gather_z1(0)
        gather_z2(0)
    with jax.named_scope("near_old"):
        gather_near(0, 0, True)
        gather_near(0, -1, True)
        gather_near(0, 1, True)
        gather_near(0, -2, True)
        gather_near(0, 2, True)
    with jax.named_scope("rz1"):
        reduce_z(1)
    with jax.named_scope("rz2"):
        reduce_z(2)
    with jax.named_scope("gz3_old"):
        gather_z3(0)
        gather_near(0, -3, True)
        gather_near(0, 3, True)
    with jax.named_scope("rl0"):
        reduce_last(0)
    with jax.named_scope("rl1"):
        reduce_last(1)
    with jax.named_scope("z4_old"):
        gather_z4(0)
        gather_near(0, 4, True)
    with jax.named_scope("rl2"):
        reduce_last(2)
    with jax.named_scope("finish"):
        finish(0)
        finish(1)
        finish(2)

    g_sum = grad[...]
    nb[0] = jnp.zeros((1, 128), F32) + jnp.sum(g_sum * g_sum)
    for d in range(1, 16):
        send(nb.at[0], nl.at[0, d], S_N, R_N, plane_peers[d - 1])
    nl[0, 0] = nb[0]
    with jax.named_scope("gfar_old"):
        gather_far(0, 0, -1, 1, -2, 2, -3, 3, 4)
    with jax.named_scope("n0"):
        received(nl.at[0, pl.ds(1, 15)], R_N)
    plane_sum = jnp.sum(nl[0], axis=0)
    nb[1] = plane_sum
    for d in range(1, 16):
        send(nb.at[1], nl.at[1, d], S_N + 1, R_N + 1, line_peers[d - 1])
    nl[1, 0] = plane_sum
    with jax.named_scope("glast_old"):
        gather_last(0, 0, -1, 1, -2, 2, -3, 3, 4)
    with jax.named_scope("n1"):
        received(nl.at[1, pl.ds(1, 15)], R_N + 1)
    square_sum = jnp.max(jnp.sum(nl[1], axis=0), axis=(0, 1), keepdims=True)
    max_norm = math.sqrt(float(CIN * TAPS * COUT))
    clip = jnp.minimum(1.0, max_norm / (jnp.sqrt(square_sum) + norm_eps))
    scaled = g_sum * clip.reshape(1, 1, 1)
    old = master[...]
    loads[0].wait()
    loads[1].wait()
    new_one = beta_one * one[...] + (1.0 - beta_one) * scaled
    new_two = beta_two * two[...] + (1.0 - beta_two) * scaled * scaled
    first_hat = new_one / (1.0 - beta_one**step_count)
    second_hat = new_two / (1.0 - beta_two**step_count)
    new_master = old - learn_rate * (
        first_hat / (jnp.sqrt(second_hat) + adam_eps) + decay_rate * old
    )
    left(wl.at[0, pl.ds(0, 7)], S_LAST)
    wf[0] = new_master[:, :, 0:256]
    wf[1] = new_master[:, :, 256:512]
    gather_start(1)
    out_master[...] = new_master
    out_one[...] = new_one
    out_two[...] = new_two
    out_grad[...] = scaled
    with jax.named_scope("gend_old"):
        gather_end(0)
    with jax.named_scope("natural_old"):

        @pl.loop(0, 9)
        def _(tap):
            natural(perm, old_m, old_o, wn, core, tap)

    with jax.named_scope("gz"):
        gather_z(1)
    with jax.named_scope("input0"):
        input_part(0)
    with jax.named_scope("input1"):
        input_part(1)
    with jax.named_scope("gz1"):
        gather_z1(1)
    with jax.named_scope("input2"):
        input_part(2)
    with jax.named_scope("gz2"):
        gather_z2(1)
        gather_far(1, 0)
    with jax.named_scope("input3"):
        input_part(3)
    with jax.named_scope("gz3"):
        gather_z3(1)
    with jax.named_scope("gfar1"):
        gather_far(1, -1, 1)
        gather_last(1, 0)
    with jax.named_scope("gz4"):
        gather_z4(1)
    with jax.named_scope("gfar2"):
        gather_far(1, -2, 2)
        gather_last(1, -1, 1)
    with jax.named_scope("gfar3"):
        gather_far(1, -3, 3, 4)
    with jax.named_scope("glast"):
        gather_last(1, -2, 2, -3, 3, 4)
    with jax.named_scope("gend"):
        gather_end(1)
    with jax.named_scope("ends"):
        left(edge_in, S_EDGE)
        left(hal, S_SLAB)
        for g in range(3):
            left(g_l.at[g], S_PAIR + g)
            left(lh.at[g], S_AH + g)
            left(lu.at[g], S_AU + g)
            left(l2.at[g], S_Z + g)
            left(fl.at[g, pl.ds(1, 7)], S_F + g)
        for k in range(2):
            left(nl.at[k, pl.ds(1, 15)], S_N + k)
        gather_left(0)
        gather_left(1)
        left(wl.at[1, pl.ds(0, 7)], S_EACH + S_LAST)


def per_device(activations, upstream, master, moment_one, moment_two):
    fields = [
        pltpu.with_memory_space_constraint(jnp.transpose(v, (1, 0, 2, 3)), pltpu.VMEM)
        for v in (activations, upstream)
    ]
    state = [jnp.transpose(v, (1, 0, 2)) for v in (master, moment_one, moment_two)]
    vmem = pl.BlockSpec(memory_space=pltpu.VMEM)
    far = pl.BlockSpec(memory_space=pl.ANY)
    shard = jax.ShapeDtypeStruct((9, 2, 512), F32)
    block = pltpu.VMEM((4, 8, 9, 16, 256), BF16)
    held = pltpu.VMEM((9, 2, 512), F32)
    input_grad, *rest = pl.pallas_call(
        kernel,
        out_shape=(
            pltpu.VMEM((4, 4, 90, 512), BF16), block, block,
            held, held, held, held,
        ),
        in_specs=[vmem, vmem, vmem, far, far],
        out_specs=(vmem,) * 7,
        scratch_shapes=[
            pltpu.VMEM((9, 2, 512), F32),
            pltpu.VMEM((9, 2, 512), F32),
            pltpu.VMEM((6, 4, 96, 512), BF16),
            pltpu.VMEM((4, 4, 96, 512), BF16),
            pltpu.VMEM((3, 512, 1536), BF16),
            pltpu.VMEM((3, 512, 1536), BF16),
            pltpu.VMEM((2, 256, 256), BF16),
            pltpu.VMEM((2, 16, 512), F32),
            pltpu.VMEM((2, 16, 512), BF16),
            pltpu.VMEM((2, 3, 16, 512), BF16),
            pltpu.VMEM((2, 4, 90, 512), BF16),
            pltpu.VMEM((3, 3, 512, 256), F32),
            pltpu.VMEM((2, 3, 512, 256), F32),
            pltpu.VMEM((3, 3, 512, 256), BF16),
            pltpu.VMEM((3, 3, 512, 256), BF16),
            pltpu.VMEM((3, 2, 3, 64, 256), BF16),
            pltpu.VMEM((3, 2, 3, 64, 256), BF16),
            pltpu.VMEM((3, 2, 3, 128, 256), BF16),
            pltpu.VMEM((3, 2, 3, 128, 256), BF16),
            pltpu.VMEM((3, 8, 3, 16, 256), F32),
            pltpu.VMEM((3, 8, 3, 16, 256), BF16),
            pltpu.VMEM((3, 7, 3, 16, 256), BF16),
            pltpu.VMEM((3, 2, 4, 3, 2, 256), F32),
            pltpu.VMEM((3, 8, 3, 2, 256), F32),
            pltpu.VMEM((9, 2, 512), F32),
            pltpu.VMEM((2, 1, 128), F32),
            pltpu.VMEM((2, 16, 1, 128), F32),
            pltpu.VMEM((2, 9, 2, 256), F32),
            pltpu.VMEM((2, 8, 9, 2, 256), F32),
            pltpu.VMEM((9, 16, 256), F32),
            pltpu.VMEM((4, 8, 9, 16, 256), BF16),
            pltpu.VMEM((4, 8, 9, 16, 256), BF16),
            pltpu.VMEM((9, 512, 512), BF16),
            pltpu.VMEM((3, 4, 104, 512), F32),
            pltpu.SemaphoreType.DMA((2,)),
            pltpu.SemaphoreType.DMA((S_LAST + 2 * S_EACH,)),
            pltpu.SemaphoreType.DMA((R_LAST + 2 * R_EACH,)),
        ],
        compiler_params=pltpu.CompilerParams(
            collective_id=0, has_side_effects=True, vmem_limit_bytes=53 * 1024 * 1024
        ),
        name="conv_step",
    )(*fields, *state)
    outs = pl.pallas_call(
        finish_kernel,
        out_shape=(jax.ShapeDtypeStruct((9, 512, 512), BF16), shard, shard, shard, shard),
        in_specs=[vmem] * 6,
        out_specs=(far,) * 5,
        scratch_shapes=[
            pltpu.VMEM((9, 512, 512), BF16),
            pltpu.VMEM((2, 256, 256), BF16),
            pltpu.SemaphoreType.DMA((13,)),
        ],
        compiler_params=pltpu.CompilerParams(vmem_limit_bytes=8 * 1024 * 1024),
        name="finish_step",
    )(*rest)
    outs = [jnp.transpose(v, (1, 0, 2)) for v in outs]
    return (jnp.transpose(input_grad, (1, 0, 2, 3)), *outs)


def solution(mesh):
    field = P(None, "lat", "lon", None)
    state = P(("lat", "lon"), None, None)
    return jax.shard_map(
        per_device,
        mesh=mesh,
        in_specs=(field, field, state, state, state),
        out_specs=(field, P(), state, state, state, state),
        check_vma=False,
    )
```
